32 devices in a mesh: gx: 2 (over core), gy: 4 (over y, x), gz: 4 (over z).
Axes of the slice: x: 2, y: 2, z: 4, core: 2. Of those that a mesh axis runs over, the one named last changes fastest.
Arguments:
- right_side: float32 [3, 32, 64, 512], P(None, 'gx', 'gy', 'gz'), may hold values from -64 to 64
- damage: int32 [32, 64, 512], P('gx', 'gy', 'gz'), may hold values from 0 to 15
Outputs:
- displacement: float32 [3, 32, 64, 512], P(None, 'gx', 'gy', 'gz')
- norms: float32 [2], replicated
The draws below stay inside these ranges and needn't reach their ends.
All inputs are finite; a program needn't handle non-finite values.
Results may differ from the reference program's by a relative error of at most 0.0003.
Values sent between devices are 32-bit elements; how exact they have to be, the bound alone decides.
A program may use at most 64 MiB of HBM per device.

```python
import math
import jax
import jax.numpy as jnp
from jax import lax

BLOCK = 16
COARSE = 8
NX = 32
NY = 64
NZ = 512


def draw_right_side(key, part):
    key_noise = jax.random.fold_in(key, 11)
    key_rows = jax.random.fold_in(key, 12)
    key_cols = jax.random.fold_in(key, 13)
    ramp = 1.0 + 2.0 * jnp.arange(NX, dtype=jnp.float32) / NX
    rough_rows = jnp.exp(jax.random.uniform(key_rows, (NX,), jnp.float32, 0.0, math.log(3.0)))
    rough_cols = jnp.exp(jax.random.uniform(key_cols, (NY,), jnp.float32, 0.0, math.log(3.0)))
    scale = (ramp * rough_rows)[:, None, None] * rough_cols[None, :, None]
    noise = jnp.clip(jax.random.normal(key_noise, (3, NX, NY, NZ), jnp.float32), -6.0, 6.0)
    return jnp.clip(noise * scale, -64.0, 64.0)


def place_ends(drawn, key, low, high):
    dims = drawn.shape
    index_at = [jax.random.randint(jax.random.fold_in(key, axis), (), 0, dims[axis]) for axis in range(len(dims))]
    drawn = drawn.at[tuple(index_at)].set(low)
    longest = dims.index(max(dims))
    index_at[longest] = (index_at[longest] + 1) % dims[longest]
    return drawn.at[tuple(index_at)].set(high)


def setup_inputs(seed: int = 0) -> dict:
    splits = jax.random.split(jax.random.key(seed), 3)
    return {
        "right_side": draw_right_side(jax.random.fold_in(splits[2], 71), 0),
        "damage": place_ends(jax.random.randint(splits[1], (NX, NY, NZ), 0, 16), jax.random.fold_in(splits[1], 1), 0, 15).astype(jnp.int32),
    }


FLOOR_STIFFNESS = 0.05
MASS_TERM = 0.001
COUPLING = 2.5
RELAXATION = 0.6

def stiffness_of(damage):
    damage_level = damage.astype(jnp.float32) / 15.0
    return (1.0 - damage_level) ** 2 * (1.0 - FLOOR_STIFFNESS) + FLOOR_STIFFNESS

def diagonal_of(coefficient, mass_term):
    return coefficient * (6.0 + 2.0 * COUPLING) + mass_term

def stencil(padded, coefficient, mass_term):
    extent = (padded.shape[1] - 2, padded.shape[2] - 2, padded.shape[3] - 2)

    def neighbour(component, offset):
        return padded[component, 1 + offset[0]:1 + offset[0] + extent[0], 1 + offset[1]:1 + offset[1] + extent[1], 1 + offset[2]:1 + offset[2] + extent[2]]

    def joined(first, second, factor):
        return tuple((first[number] + factor * second[number] for number in range(3)))
    unit_steps = ((1, 0, 0), (0, 1, 0), (0, 0, 1))
    images = []
    for component in range(3):
        centre = neighbour(component, (0, 0, 0))
        beside_all = jnp.zeros_like(centre)
        for partner in range(3):
            step_up = unit_steps[partner]
            step_down = joined((0, 0, 0), step_up, -1)
            beside_all = beside_all + neighbour(component, step_up) + neighbour(component, step_down)
        own_up = unit_steps[component]
        own_down = joined((0, 0, 0), own_up, -1)
        axial_part = 2.0 * centre - neighbour(component, own_up) - neighbour(component, own_down)
        mixed_part = jnp.zeros_like(centre)
        for partner in range(3):
            if partner != component:
                other_up = unit_steps[partner]
                mixed_part = mixed_part + neighbour(partner, joined(own_up, other_up, 1)) - neighbour(partner, joined(own_up, other_up, -1)) - neighbour(partner, joined(own_down, other_up, 1)) + neighbour(partner, joined(own_down, other_up, -1))
        images.append(coefficient * (6.0 * centre - beside_all + COUPLING * (axial_part - 0.25 * mixed_part)) + mass_term * centre)
    return jnp.stack(images)

def apply_whole(displacement, coefficient):
    padded = jnp.pad(displacement, ((0, 0), (1, 1), (1, 1), (1, 1)))
    block_count = displacement.shape[1] // BLOCK

    def one_block(block_no):
        start = (block_no * BLOCK).astype(jnp.int32)
        slab_piece = lax.dynamic_slice_in_dim(padded, start, BLOCK + 2, 1)
        slab_stiff = lax.dynamic_slice_in_dim(coefficient, start, BLOCK, 0)
        return stencil(slab_piece, slab_stiff, MASS_TERM)
    blocks_out = lax.map(one_block, jnp.arange(block_count, dtype=jnp.int32))
    return jnp.moveaxis(blocks_out, 0, 1).reshape(displacement.shape)

def block_sums(source):
    channels, size_x, size_y, size_z = source.shape
    return lax.optimization_barrier(jnp.sum(source.reshape(channels, size_x // BLOCK, BLOCK, size_y // BLOCK, BLOCK, size_z // BLOCK, BLOCK), axis=(2, 4, 6)))

def spread(block_field):
    channels, size_x, size_y, size_z = block_field.shape
    widened = jnp.broadcast_to(block_field[:, :, None, :, None, :, None], (channels, size_x, BLOCK, size_y, BLOCK, size_z, BLOCK))
    return widened.reshape(channels, size_x * BLOCK, size_y * BLOCK, size_z * BLOCK)

def coarse_sweeps(coarse_load, mean_stiffness):
    coarse_coefficient = BLOCK ** 2 * mean_stiffness
    coarse_mass = BLOCK ** 3 * MASS_TERM
    coarse_diagonal = diagonal_of(coarse_coefficient, coarse_mass)
    correction = RELAXATION * coarse_load / coarse_diagonal
    for repeat in range(COARSE - 1):
        padded = jnp.pad(correction, ((0, 0), (1, 1), (1, 1), (1, 1)))
        coarse_image = stencil(padded, coarse_coefficient, coarse_mass)
        correction = correction + RELAXATION * (coarse_load - coarse_image) / coarse_diagonal
    return correction

def reference(right_side, damage):
    coefficient = stiffness_of(damage)
    diagonal = diagonal_of(coefficient, MASS_TERM)
    displacement = RELAXATION * right_side / diagonal
    displacement = displacement + RELAXATION * (right_side - apply_whole(displacement, coefficient)) / diagonal
    residual = right_side - apply_whole(displacement, coefficient)
    coarse_load = block_sums(residual)
    mean_stiffness = (block_sums(coefficient[None]) / BLOCK ** 3)[0]
    correction = coarse_sweeps(coarse_load, mean_stiffness)
    displacement = displacement + spread(correction)
    for repeat in range(2):
        displacement = displacement + RELAXATION * (right_side - apply_whole(displacement, coefficient)) / diagonal
    residual = right_side - apply_whole(displacement, coefficient)
    total_count = 3 * NX * NY * NZ
    load_sum = jnp.sum(right_side * right_side)
    residual_sum = jnp.sum(residual * residual)
    norms = jnp.stack([jnp.sqrt(load_sum / total_count), jnp.sqrt(residual_sum / total_count)])
    return (displacement, norms)
```

```python
import functools

import jax
import jax.numpy as jnp
from jax import lax
from jax.experimental import pallas as pl
from jax.experimental.pallas import tpu as pltpu
from jax.sharding import PartitionSpec as P

BLOCK = 16
COARSE = 8
FLOOR_STIFFNESS = 0.05
MASS_TERM = 0.001
COUPLING = 2.5
RELAXATION = 0.6
DIAGONAL = 6.0 + 2.0 * COUPLING
OWN = 1.0 + COUPLING
CROSS = 0.25 * COUPLING
AXES = ("gx", "gy", "gz")
HALO = 4
LANES = 128
MESH = pl.DeviceIdType.MESH
EXACT = lax.Precision.HIGHEST


def messages():
    out = []
    for dx in (-1, 1):
        for part in range(HALO):
            out.append(("x", dx, 0, 0, part))
    for part in range(2):
        for dy in (-1, 1):
            out.append(("y", 0, dy, 0, part))
        for dx in (-1, 1):
            for dy in (-1, 1):
                out.append(("xy", dx, dy, 0, part))
        if part == 0:
            for dz in (-1, 1):
                for dx in (-1, 0, 1):
                    for dy in (-1, 0, 1):
                        out.append(("z" if dx == 0 else "xz", dx, dy, dz, 0))
    return out


MESSAGES = messages()


def kernel(
    counts,
    extent,
    load_ref,
    damage_ref,
    out_ref,
    norms_ref,
    base,
    inverse,
    field_a,
    field_b,
    harm,
    y_send,
    y_recv,
    xy_send,
    xy_recv,
    z_send,
    z_recv,
    xz_send,
    xz_recv,
    coarse_send,
    coarse_recv,
    coarse_w,
    spread_w,
    norm_send,
    norm_recv,
    local_sem,
    send_sem,
    recv_sem,
    coarse_send_sem,
    coarse_recv_sem,
    norm_send_sem,
    norm_recv_sem,
):
    count_x, count_y, count_z = counts
    ex, ey, ez = extent
    cz = ez // BLOCK
    total = count_x * count_y * count_z
    wide_x = ex + 2 * HALO
    ypad = 8
    rows = ey + 2 * ypad
    wide_y = ey + 2 * HALO
    first_y = ypad - HALO
    me = tuple(lax.axis_index(axis) for axis in AXES)
    my_id = (me[0] * count_y + me[1]) * count_z + me[2]

    def place(index):
        return (
            index // (count_y * count_z),
            lax.rem(index // count_z, count_y),
            lax.rem(index, count_z),
        )

    load_copies = []
    for x in range(ex):
        target = pl.ds((HALO + x) * rows + ypad, ey)
        load_copies.append(
            pltpu.make_async_copy(load_ref.at[:, x], base.at[0, 0:3, target], local_sem.at[x])
        )
    harm_copy = pltpu.make_async_copy(damage_ref, harm, local_sem.at[ex])
    harm_copy.start()
    for copy in load_copies:
        copy.start()

    barrier = pltpu.get_barrier_semaphore()

    def greet(step, carry):
        pl.semaphore_signal(
            barrier,
            inc=1,
            device_id=place(lax.rem(my_id + step, total)),
            device_id_type=MESH,
        )
        return carry

    lax.fori_loop(1, total, greet, 0)

    harm_copy.wait()
    for x in range(ex):
        level = 1.0 - harm[x].astype(jnp.float32) / 15.0
        base[0, 3, pl.ds((HALO + x) * rows + ypad, ey)] = (
            level * level * (1.0 - FLOOR_STIFFNESS) + FLOOR_STIFFNESS
        )
    for copy in load_copies:
        copy.wait()

    lane = lax.broadcasted_iota(jnp.int32, (ey, LANES), 1)
    for side in range(2):
        for part in range(2):
            for layer in range(2):
                y = 2 * part + layer if side == 0 else ey - 2 - 2 * part + layer
                for f in range(4):
                    start = HALO * rows + ypad + y
                    for half in range(ex // 8):
                        y_send[side, part, f, layer, pl.ds(8 * half, 8)] = base[
                            0, f, pl.ds(start + 8 * half * rows, 8, stride=rows)
                        ]
                    for xs in range(2):
                        x0 = 0 if xs == 0 else ex - HALO
                        xy_send[xs, side, part, f, layer] = base[
                            0, f, pl.ds(start + x0 * rows, HALO, stride=rows)
                        ]
    for f in range(4):
        packed = None
        for k in range(ex):
            row = base[0, f, pl.ds((HALO + k) * rows + ypad, ey)]
            moved = pltpu.roll(row, (8 * k + HALO) % LANES, 1)
            packed = moved if packed is None else jnp.where(lane // 8 == k, moved, packed)
        z_send[f] = packed
    for xs in range(2):
        packed = None
        for f in range(4):
            for j in range(HALO):
                x = j if xs == 0 else ex - HALO + j
                k = f * HALO + j
                row = base[0, f, pl.ds((HALO + x) * rows + ypad, ey)]
                moved = pltpu.roll(row, (8 * k + HALO) % LANES, 1)
                packed = moved if packed is None else jnp.where(lane // 8 == k, moved, packed)
        xz_send[xs] = packed

    pl.semaphore_wait(barrier, total - 1)

    def exists(dx, dy, dz):
        ok = None
        for axis, step in enumerate((dx, dy, dz)):
            if step == 0:
                continue
            here = me[axis] + step
            good = (here >= 0) & (here < counts[axis])
            ok = good if ok is None else ok & good
        return ok

    def describe(number):
        kind, dx, dy, dz, part = MESSAGES[number]
        target = (me[0] + dx, me[1] + dy, me[2] + dz)
        xs, ys, zs = (dx + 1) // 2, (dy + 1) // 2, (dz + 1) // 2
        if kind == "x":
            src_x = HALO + part if dx < 0 else ex + part
            dst_x = HALO + ex + part if dx < 0 else part
            src = base.at[0, :, pl.ds(src_x * rows + ypad, ey)]
            dst = base.at[0, :, pl.ds(dst_x * rows + ypad, ey)]
        elif kind == "y":
            src, dst = y_send.at[ys, part], y_recv.at[1 - ys, part]
        elif kind == "xy":
            src, dst = xy_send.at[xs, ys, part], xy_recv.at[1 - xs, 1 - ys, part]
        else:
            if dy == 0:
                src_y, dst_y, size = 0, ypad, ey
            elif dy < 0:
                src_y, dst_y, size = 0, ypad + ey, ypad
            else:
                src_y, dst_y, size = ey - ypad, 0, ypad
            if kind == "z":
                src = z_send.at[:, pl.ds(src_y, size)]
                dst = z_recv.at[1 - zs, :, pl.ds(dst_y, size)]
            else:
                src = xz_send.at[xs, pl.ds(src_y, size)]
                dst = xz_recv.at[1 - xs, 1 - zs, pl.ds(dst_y, size)]
        copy = pltpu.make_async_remote_copy(
            src_ref=src,
            dst_ref=dst,
            send_sem=send_sem.at[number],
            recv_sem=recv_sem.at[number],
            device_id=target,
            device_id_type=MESH,
        )
        return copy, exists(dx, dy, dz), exists(-dx, -dy, -dz)

    for number in range(len(MESSAGES)):
        copy, to_there, _ = describe(number)

        @pl.when(to_there)
        def _():
            copy.start()

    def wait_for(part, send):
        for number, message in enumerate(MESSAGES):
            far = message[0] in ("y", "xy") and message[4] == 1
            if send and (message[0] == "x") != (part == 0):
                continue
            if not send and far != (part == 1):
                continue
            copy, to_there, from_there = describe(number)

            @pl.when(to_there if send else from_there)
            def _():
                if send:
                    copy.wait_send()
                else:
                    copy.wait_recv()

    def unpack_y(part):
        for side in range(2):
            for layer in range(2):
                y = (
                    ypad - 2 - 2 * part + layer
                    if side == 0
                    else ypad + ey + 2 * part + layer
                )
                for f in range(4):
                    for half in range(ex // 8):
                        base[
                            0, f, pl.ds((HALO + 8 * half) * rows + y, 8, stride=rows)
                        ] = y_recv[side, part, f, layer, pl.ds(8 * half, 8)]
                    for xs in range(2):
                        x0 = 0 if xs == 0 else HALO + ex
                        base[0, f, pl.ds(x0 * rows + y, HALO, stride=rows)] = xy_recv[
                            xs, side, part, f, layer
                        ]

    def unpack_z():
        lane_rows = lax.broadcasted_iota(jnp.int32, (rows, LANES), 1)
        lower = lax.rem(lane_rows, 8) < HALO
        for f in range(4):
            merged = jnp.where(lower, z_recv[0, f], z_recv[1, f])
            for k in range(ex):
                base[1, f, pl.ds((HALO + k) * rows, rows)] = pltpu.roll(
                    merged, (2 * LANES - 8 * k - HALO) % LANES, 1
                )
        for xs in range(2):
            merged = jnp.where(lower, xz_recv[xs, 0], xz_recv[xs, 1])
            for f in range(4):
                for j in range(HALO):
                    k = f * HALO + j
                    x = j if xs == 0 else HALO + ex + j
                    base[1, f, pl.ds(x * rows, rows)] = pltpu.roll(
                        merged, (2 * LANES - 8 * k - HALO) % LANES, 1
                    )

    lane = lax.broadcasted_iota(jnp.int32, (wide_y, LANES), 1)
    row_y = lax.broadcasted_iota(jnp.int32, (wide_y, LANES), 0)
    at_y = me[1] * ey + row_y - HALO
    good_y = (at_y >= 0) & (at_y < ey * count_y)
    good_halo = (
        good_y
        & ((me[2] > 0) | (lane < LANES // 2))
        & ((me[2] < count_z - 1) | (lane >= LANES // 2))
    )
    goods = (good_y, good_halo)

    def at(x, dy=0):
        return pl.ds(x * rows + first_y + dy, wide_y)

    def prepare(x, carry):
        at_x = me[0] * ex + x - HALO
        good_x = (at_x >= 0) & (at_x < ex * count_x)
        for t in range(2):
            good = goods[t] & good_x
            g = jnp.where(good, base[t, 3, at(x)], 1.0)
            base[t, 3, at(x)] = g
            inv = jnp.where(good, RELAXATION / (g * DIAGONAL + MASS_TERM), 0.0)
            inverse[t, at(x)] = inv
            for c in range(3):
                load = jnp.where(good, base[t, c, at(x)], 0.0)
                base[t, c, at(x)] = load
                field_a[t, c, at(x)] = load * inv
        return carry

    first_lane = lane == 0
    last_lane = lane == LANES - 1

    def image(field, x):
        parts = [[None] * 3, [None] * 3]
        ups = [[None] * 3, [None] * 3]
        downs = [[None] * 3, [None] * 3]
        for t in range(2):

            def load(c, ox, oy):
                return field[t, c, at(x + ox, oy)]

            centre = [load(c, 0, 0) for c in range(3)]
            x_up = [load(c, 1, 0) for c in range(3)]
            x_down = [load(c, -1, 0) for c in range(3)]
            y_up = [load(c, 0, 1) for c in range(3)]
            y_down = [load(c, 0, -1) for c in range(3)]

            def corners(c):
                return (load(c, 1, 1) - load(c, 1, -1)) - (load(c, -1, 1) - load(c, -1, -1))

            sum_x = [x_up[c] + x_down[c] for c in range(3)]
            sum_y = [y_up[c] + y_down[c] for c in range(3)]
            parts[t][0] = DIAGONAL * centre[0] - OWN * sum_x[0] - sum_y[0] - CROSS * corners(1)
            parts[t][1] = DIAGONAL * centre[1] - sum_x[1] - OWN * sum_y[1] - CROSS * corners(0)
            parts[t][2] = DIAGONAL * centre[2] - sum_x[2] - sum_y[2]
            tilt_x = CROSS * (x_up[2] - x_down[2])
            tilt_y = CROSS * (y_up[2] - y_down[2])
            tilt_z = CROSS * ((x_up[0] - x_down[0]) + (y_up[1] - y_down[1]))
            own_z = OWN * centre[2]
            ups[t] = [centre[0] + tilt_x, centre[1] + tilt_y, own_z + tilt_z]
            downs[t] = [centre[0] - tilt_x, centre[1] - tilt_y, own_z - tilt_z]
        out = [[None] * 3, [None] * 3]
        for c in range(3):
            up = [pltpu.roll(ups[t][c], LANES - 1, 1) for t in range(2)]
            down = [pltpu.roll(downs[t][c], 1, 1) for t in range(2)]
            for t in range(2):
                beside = jnp.where(last_lane, up[1 - t], up[t]) + jnp.where(
                    first_lane, down[1 - t], down[t]
                )
                out[t][c] = parts[t][c] - beside
        return out

    def residual(field, x, tiles):
        images = image(field, x)
        out = []
        for t in tiles:
            g = base[t, 3, at(x)]
            out.append(
                [
                    base[t, c, at(x)] - (g * images[t][c] + MASS_TERM * field[t, c, at(x)])
                    for c in range(3)
                ]
            )
        return out

    def sweep(source, target, low, high):
        def one(x, carry):
            left = residual(source, x, (0, 1))
            for t in range(2):
                inv = inverse[t, at(x)]
                for c in range(3):
                    target[t, c, at(x)] = source[t, c, at(x)] + inv * left[t][c]
            return carry

        lax.fori_loop(low, high, one, 0)

    inner_y = (row_y >= HALO) & (row_y < HALO + ey)

    def fold(value):
        return jnp.sum(value.reshape(wide_y // 8, 8, LANES), axis=0)

    zero = jnp.zeros((8, LANES), jnp.float32)

    wait_for(0, False)
    wait_for(0, True)
    unpack_y(0)
    unpack_z()
    lax.fori_loop(2, wide_x - 2, prepare, 0)
    sweep(field_a, field_b, 3, wide_x - 3)

    def restrict(x, carry):
        left = residual(field_b, x, (0,))[0]
        sums = [
            carry[c] + fold(jnp.where(inner_y, left[c], 0.0)) for c in range(3)
        ]
        sums.append(carry[3] + fold(jnp.where(inner_y, base[0, 3, at(x)], 0.0)))
        return tuple(sums)

    sums = lax.fori_loop(HALO, HALO + ex, restrict, (zero,) * 4)
    stacked = jnp.concatenate([jnp.sum(s, axis=0, keepdims=True) for s in sums] + [zero[:4]], axis=0)
    source_lane = lax.broadcasted_iota(jnp.int32, (LANES, LANES), 0)
    target_lane = lax.broadcasted_iota(jnp.int32, (LANES, LANES), 1)
    gather = (source_lane // BLOCK == lax.rem(target_lane, cz)).astype(jnp.float32)
    grouped = jnp.dot(stacked, gather, precision=EXACT, preferred_element_type=jnp.float32)
    coarse_send[...] = grouped[:4]

    reach = -(-COARSE // cz)
    window = 2 * reach + 1

    def peers(act):
        for dz in range(-reach, reach + 1):
            z = me[2] + dz

            @pl.when((z >= 0) & (z < count_z))
            def _():
                def one(step, carry):
                    if dz == 0:
                        step = step + 1
                    index = lax.rem(me[0] * count_y + me[1] + step, count_x * count_y)
                    act(index // count_y, lax.rem(index, count_y), z, dz)
                    return carry

                lax.fori_loop(0, count_x * count_y - (1 if dz == 0 else 0), one, 0)

    def coarse_copy(x, y, z, dz):
        return pltpu.make_async_remote_copy(
            src_ref=coarse_send,
            dst_ref=coarse_recv.at[reach - dz, me[0], me[1]],
            send_sem=coarse_send_sem.at[reach + dz, x, y],
            recv_sem=coarse_recv_sem.at[reach - dz, me[0], me[1]],
            device_id=(x, y, z),
            device_id_type=MESH,
        )

    def coarse_wait(x, y, z, dz):
        pltpu.make_async_remote_copy(
            src_ref=coarse_send,
            dst_ref=coarse_recv.at[reach + dz, x, y],
            send_sem=coarse_send_sem.at[reach + dz, x, y],
            recv_sem=coarse_recv_sem.at[reach + dz, x, y],
            device_id=(x, y, z),
            device_id_type=MESH,
        ).wait()

    peers(lambda x, y, z, dz: coarse_copy(x, y, z, dz).start())
    coarse_recv[reach, me[0], me[1]] = grouped[:4]

    wait_for(1, False)
    unpack_y(1)
    lax.fori_loop(0, wide_x, prepare, 0)
    sweep(field_a, field_b, 1, wide_x - 1)
    wait_for(1, True)
    peers(coarse_wait)

    coarse_rows = -(-(count_y + 1) // 8) * 8
    lane_c = lax.broadcasted_iota(jnp.int32, (coarse_rows, LANES), 1)
    row_c = lax.broadcasted_iota(jnp.int32, (coarse_rows, LANES), 0)
    at_z = me[2] * cz - reach * cz + lane_c
    valid = (
        (row_c < count_y) & (at_z >= 0) & (at_z < cz * count_z) & (lane_c < window * cz)
    )
    slab = [[None] * 4 for _ in range(count_x)]
    for x in range(count_x):
        for c in range(4):
            value = None
            for w in range(window):
                column = jnp.concatenate(
                    [coarse_recv[w, x, y, c : c + 1] for y in range(count_y)]
                    + [jnp.zeros((coarse_rows - count_y, LANES), jnp.float32)],
                    axis=0,
                )
                value = column if value is None else jnp.where(lane_c // cz == w, column, value)
            slab[x][c] = jnp.where(valid, value, 0.0)
    mass = BLOCK**3 * MASS_TERM
    factor = [slab[x][3] * (BLOCK**2 / BLOCK**3) for x in range(count_x)]
    relax = [
        jnp.where(valid, RELAXATION / (factor[x] * DIAGONAL + mass), 0.0) for x in range(count_x)
    ]
    nothing = jnp.zeros((coarse_rows, LANES), jnp.float32)
    w = [[slab[x][c] * relax[x] for c in range(3)] for x in range(count_x)]

    def y_shift(value, step):
        return pltpu.roll(value, step % coarse_rows, 0)

    def z_shift(value, step):
        return pltpu.roll(value, step % LANES, 1)

    for repeat in range(COARSE - 1):
        fresh = []
        for x in range(count_x):
            here = w[x]
            above = w[x + 1] if x + 1 < count_x else [nothing] * 3
            below = w[x - 1] if x > 0 else [nothing] * 3
            sum_x = [above[c] + below[c] for c in range(3)]
            diff_x = [above[c] - below[c] for c in range(3)]
            y_up = [y_shift(here[c], -1) for c in range(3)]
            y_down = [y_shift(here[c], 1) for c in range(3)]
            sum_y = [y_up[c] + y_down[c] for c in range(3)]
            diff_y = [y_up[c] - y_down[c] for c in range(3)]
            corner_x = y_shift(diff_x[1], -1) - y_shift(diff_x[1], 1)
            corner_y = y_shift(diff_x[0], -1) - y_shift(diff_x[0], 1)
            tilt = [CROSS * diff_x[2], CROSS * diff_y[2], CROSS * (diff_x[0] + diff_y[1])]
            own = [here[0], here[1], OWN * here[2]]
            beside = [z_shift(own[c] + tilt[c], -1) + z_shift(own[c] - tilt[c], 1) for c in range(3)]
            flat = [
                DIAGONAL * here[0] - OWN * sum_x[0] - sum_y[0] - CROSS * corner_x - beside[0],
                DIAGONAL * here[1] - sum_x[1] - OWN * sum_y[1] - CROSS * corner_y - beside[1],
                DIAGONAL * here[2] - sum_x[2] - sum_y[2] - beside[2],
            ]
            fresh.append(
                [
                    here[c] + relax[x] * (slab[x][c] - (factor[x] * flat[c] + mass * here[c]))
                    for c in range(3)
                ]
            )
        w = fresh

    for x in range(count_x + 2):
        for c in range(3):
            inside = 1 <= x <= count_x
            coarse_w[x, c, pl.ds(0, 8)] = jnp.zeros((8, LANES), jnp.float32)
            coarse_w[x, c, pl.ds(8, coarse_rows)] = w[x - 1][c] if inside else nothing
    widen_core = (source_lane == reach * cz + target_lane // BLOCK).astype(jnp.float32)
    widen_halo = (
        source_lane == jnp.where(target_lane < LANES // 2, (reach + 1) * cz, reach * cz - 1)
    ).astype(jnp.float32)
    for xc in range(3):
        for c in range(3):
            cells = [coarse_w[me[0] + xc, c, pl.ds(7 + me[1] + k, 1)] for k in range(3)]
            stacked = jnp.concatenate(cells + [zero[:5]], axis=0)
            for t, matrix in enumerate((widen_core, widen_halo)):
                wide = jnp.dot(stacked, matrix, precision=EXACT, preferred_element_type=jnp.float32)
                low = jnp.broadcast_to(wide[0:1], (wide_y, LANES))
                mid = jnp.broadcast_to(wide[1:2], (wide_y, LANES))
                top = jnp.broadcast_to(wide[2:3], (wide_y, LANES))
                spread_w[t, c, xc] = jnp.where(
                    row_y < HALO, low, jnp.where(row_y < HALO + ey, mid, top)
                )

    def correct(x, carry):
        cell = (x + ex - HALO) // ex
        for t in range(2):
            for c in range(3):
                field_b[t, c, at(x)] = field_b[t, c, at(x)] + spread_w[t, c, cell]
        return carry

    lax.fori_loop(1, wide_x - 1, correct, 0)
    sweep(field_b, field_a, 2, wide_x - 2)
    sweep(field_a, field_b, 3, wide_x - 3)
    out_copies = []
    for x in range(ex):
        copy = pltpu.make_async_copy(
            field_b.at[0, :, pl.ds((HALO + x) * rows + ypad, ey)],
            out_ref.at[:, x],
            local_sem.at[x],
        )
        copy.start()
        out_copies.append(copy)

    def squares(x, carry):
        left = residual(field_b, x, (0,))[0]
        both = []
        square = sum(value * value for value in left)
        loads = [base[0, c, at(x)] for c in range(3)]
        load_square = sum(value * value for value in loads)
        both.append(carry[0] + fold(jnp.where(inner_y, load_square, 0.0)))
        both.append(carry[1] + fold(jnp.where(inner_y, square, 0.0)))
        return tuple(both)

    load_sum, left_sum = lax.fori_loop(HALO, HALO + ex, squares, (zero, zero))
    load_total = jnp.sum(jnp.sum(load_sum, axis=0, keepdims=True), axis=1, keepdims=True)
    left_total = jnp.sum(jnp.sum(left_sum, axis=0, keepdims=True), axis=1, keepdims=True)
    first = lax.broadcasted_iota(jnp.int32, (1, LANES), 1) == 0
    mine = jnp.where(first, load_total, left_total)
    norm_send[...] = mine

    def norm_copy(step):
        return pltpu.make_async_remote_copy(
            src_ref=norm_send,
            dst_ref=norm_recv.at[step - 1],
            send_sem=norm_send_sem.at[step - 1],
            recv_sem=norm_recv_sem.at[step - 1],
            device_id=place(lax.rem(my_id + step, total)),
            device_id_type=MESH,
        )

    def norm_start(step, carry):
        norm_copy(step).start()
        return carry

    def norm_wait(step, carry):
        norm_copy(step).wait()
        return carry

    lax.fori_loop(1, total, norm_start, 0)
    norm_recv[total - 1] = mine
    for copy in out_copies:
        copy.wait()
    lax.fori_loop(1, total, norm_wait, 0)

    def add(device, carry):
        slot = lax.rem(my_id - device + total - 1, total)
        return carry + norm_recv[lax.rem(slot + total, total)]

    summed = lax.fori_loop(0, total, add, jnp.zeros((1, LANES), jnp.float32))
    nodes = 3 * ex * ey * ez * total
    norms_ref[...] = jnp.sqrt(summed / nodes)


def on_device(counts, right_side, damage):
    _, ex, ey, ez = right_side.shape
    cz = ez // BLOCK
    wide_x = ex + 2 * HALO
    rows = ey + 16
    flat = wide_x * rows
    wide_y = ey + 2 * HALO
    total = counts[0] * counts[1] * counts[2]
    window = 2 * (-(-COARSE // cz)) + 1
    coarse_rows = -(-(counts[1] + 1) // 8) * 8
    f32 = jnp.float32
    vmem = pltpu.VMEM
    dma = pltpu.SemaphoreType.DMA
    displacement, norms = pl.pallas_call(
        functools.partial(kernel, counts, (ex, ey, ez)),
        out_shape=(
            jax.ShapeDtypeStruct(right_side.shape, f32),
            jax.ShapeDtypeStruct((1, LANES), f32),
        ),
        in_specs=[pl.BlockSpec(memory_space=pl.ANY)] * 2,
        out_specs=(
            pl.BlockSpec(memory_space=pl.ANY),
            pl.BlockSpec(memory_space=pltpu.VMEM),
        ),
        scratch_shapes=[
            vmem((2, 4, flat, LANES), f32),
            vmem((2, flat, LANES), f32),
            vmem((2, 3, flat, LANES), f32),
            vmem((2, 3, flat, LANES), f32),
            vmem((ex, ey, LANES), jnp.int32),
            vmem((2, 2, 4, 2, ex, LANES), f32),
            vmem((2, 2, 4, 2, ex, LANES), f32),
            vmem((2, 2, 2, 4, 2, HALO, LANES), f32),
            vmem((2, 2, 2, 4, 2, HALO, LANES), f32),
            vmem((4, ey, LANES), f32),
            vmem((2, 4, rows, LANES), f32),
            vmem((2, ey, LANES), f32),
            vmem((2, 2, rows, LANES), f32),
            vmem((4, LANES), f32),
            vmem((window, counts[0], counts[1], 4, LANES), f32),
            vmem((counts[0] + 2, 3, 8 + coarse_rows, LANES), f32),
            vmem((2, 3, 3, wide_y, LANES), f32),
            vmem((1, LANES), f32),
            vmem((total, 1, LANES), f32),
            dma((ex + 1,)),
            dma((len(MESSAGES),)),
            dma((len(MESSAGES),)),
            dma((window, counts[0], counts[1])),
            dma((window, counts[0], counts[1])),
            dma((total,)),
            dma((total,)),
        ],
        compiler_params=pltpu.CompilerParams(collective_id=0, has_side_effects=True),
    )(right_side, damage)
    return displacement, norms[0, :2]


def solution(mesh):
    counts = tuple(mesh.shape[axis] for axis in AXES)
    placed = (P(None, "gx", "gy", "gz"), P("gx", "gy", "gz"))
    return jax.shard_map(
        functools.partial(on_device, counts),
        mesh=mesh,
        in_specs=placed,
        out_specs=(P(None, "gx", "gy", "gz"), P()),
        check_vma=False,
    )
```

```python
import functools

import jax
import jax.numpy as jnp
from jax import lax
from jax.experimental import pallas as pl
from jax.experimental.pallas import tpu as pltpu
from jax.sharding import PartitionSpec as P

BLOCK = 16
COARSE = 8
FLOOR_STIFFNESS = 0.05
MASS_TERM = 0.001
COUPLING = 2.5
RELAXATION = 0.6
DIAGONAL = 6.0 + 2.0 * COUPLING
OWN = 1.0 + COUPLING
CROSS = 0.25 * COUPLING
AXES = ("gx", "gy", "gz")
HALO = 4
LANES = 128
MESH = pl.DeviceIdType.MESH
EXACT = lax.Precision.HIGHEST


def messages():
    out = []
    for dx in (-1, 1):
        for part in range(HALO):
            out.append(("x", dx, 0, 0, part))
    for part in range(2):
        for dy in (-1, 1):
            out.append(("y", 0, dy, 0, part))
        for dx in (-1, 1):
            for dy in (-1, 1):
                out.append(("xy", dx, dy, 0, part))
        if part == 0:
            for dz in (-1, 1):
                for dx in (-1, 0, 1):
                    for dy in (-1, 0, 1):
                        out.append(("z" if dx == 0 else "xz", dx, dy, dz, 0))
    return out


MESSAGES = messages()


def kernel(
    counts,
    extent,
    load_ref,
    damage_ref,
    out_ref,
    norms_ref,
    base,
    inverse,
    field_a,
    field_b,
    harm,
    y_send,
    y_recv,
    xy_send,
    xy_recv,
    z_send,
    z_recv,
    xz_send,
    xz_recv,
    coarse_send,
    coarse_recv,
    coarse_w,
    spread_w,
    image_w,
    norm_send,
    norm_recv,
    local_sem,
    send_sem,
    recv_sem,
    coarse_send_sem,
    coarse_recv_sem,
    norm_send_sem,
    norm_recv_sem,
    hello_sem,
):
    count_x, count_y, count_z = counts
    ex, ey, ez = extent
    cz = ez // BLOCK
    total = count_x * count_y * count_z
    wide_x = ex + 2 * HALO
    ypad = 8
    rows = ey + 2 * ypad
    wide_y = ey + 2 * HALO
    first_y = ypad - HALO
    me = tuple(lax.axis_index(axis) for axis in AXES)
    my_id = (me[0] * count_y + me[1]) * count_z + me[2]

    def place(index):
        return (
            index // (count_y * count_z),
            lax.rem(index // count_z, count_y),
            lax.rem(index, count_z),
        )

    load_copies = []
    for x in range(ex):
        target = pl.ds((HALO + x) * rows + ypad, ey)
        load_copies.append(
            pltpu.make_async_copy(load_ref.at[:, x], base.at[0, 0:3, target], local_sem.at[x])
        )
    harm_copy = pltpu.make_async_copy(damage_ref, harm, local_sem.at[ex])
    harm_copy.start()
    for copy in load_copies:
        copy.start()

    barrier = pltpu.get_barrier_semaphore()

    reach = -(-COARSE // cz)
    window = 2 * reach + 1

    def peers(act):
        for dz in range(-reach, reach + 1):
            z = me[2] + dz

            @pl.when((z >= 0) & (z < count_z))
            def _():
                def one(step, carry):
                    if dz == 0:
                        step = step + 1
                    index = lax.rem(me[0] * count_y + me[1] + step, count_x * count_y)
                    act(index // count_y, lax.rem(index, count_y), z, dz)
                    return carry

                lax.fori_loop(0, count_x * count_y - (1 if dz == 0 else 0), one, 0)

    def greet(x, y, z, dz):
        pl.semaphore_signal(barrier, inc=1, device_id=(x, y, z), device_id_type=MESH)

    peers(greet)
    levels = jnp.minimum(me[2] + reach, count_z - 1) - jnp.maximum(me[2] - reach, 0) + 1

    harm_copy.wait()
    for x in range(ex):
        level = 1.0 - harm[x].astype(jnp.float32) / 15.0
        base[0, 3, pl.ds((HALO + x) * rows + ypad, ey)] = (
            level * level * (1.0 - FLOOR_STIFFNESS) + FLOOR_STIFFNESS
        )
    for copy in load_copies:
        copy.wait()

    lane = lax.broadcasted_iota(jnp.int32, (ey, LANES), 1)
    for side in range(2):
        for part in range(2):
            for layer in range(2):
                y = 2 * part + layer if side == 0 else ey - 2 - 2 * part + layer
                for f in range(4):
                    start = HALO * rows + ypad + y
                    for half in range(ex // 8):
                        y_send[side, part, f, layer, pl.ds(8 * half, 8)] = base[
                            0, f, pl.ds(start + 8 * half * rows, 8, stride=rows)
                        ]
                    for xs in range(2):
                        x0 = 0 if xs == 0 else ex - HALO
                        xy_send[xs, side, part, f, layer] = base[
                            0, f, pl.ds(start + x0 * rows, HALO, stride=rows)
                        ]
    for f in range(4):
        packed = None
        for k in range(ex):
            row = base[0, f, pl.ds((HALO + k) * rows + ypad, ey)]
            moved = pltpu.roll(row, (8 * k + HALO) % LANES, 1)
            packed = moved if packed is None else jnp.where(lane // 8 == k, moved, packed)
        z_send[f] = packed
    for xs in range(2):
        packed = None
        for f in range(4):
            for j in range(HALO):
                x = j if xs == 0 else ex - HALO + j
                k = f * HALO + j
                row = base[0, f, pl.ds((HALO + x) * rows + ypad, ey)]
                moved = pltpu.roll(row, (8 * k + HALO) % LANES, 1)
                packed = moved if packed is None else jnp.where(lane // 8 == k, moved, packed)
        xz_send[xs] = packed

    pl.semaphore_wait(barrier, levels * count_x * count_y - 1)

    def exists(dx, dy, dz):
        ok = None
        for axis, step in enumerate((dx, dy, dz)):
            if step == 0:
                continue
            here = me[axis] + step
            good = (here >= 0) & (here < counts[axis])
            ok = good if ok is None else ok & good
        return ok

    def describe(number):
        kind, dx, dy, dz, part = MESSAGES[number]
        target = (me[0] + dx, me[1] + dy, me[2] + dz)
        xs, ys, zs = (dx + 1) // 2, (dy + 1) // 2, (dz + 1) // 2
        if kind == "x":
            src_x = HALO + part if dx < 0 else ex + part
            dst_x = HALO + ex + part if dx < 0 else part
            src = base.at[0, :, pl.ds(src_x * rows + ypad, ey)]
            dst = base.at[0, :, pl.ds(dst_x * rows + ypad, ey)]
        elif kind == "y":
            src, dst = y_send.at[ys, part], y_recv.at[1 - ys, part]
        elif kind == "xy":
            src, dst = xy_send.at[xs, ys, part], xy_recv.at[1 - xs, 1 - ys, part]
        else:
            if dy == 0:
                src_y, dst_y, size = 0, ypad, ey
            elif dy < 0:
                src_y, dst_y, size = 0, ypad + ey, ypad
            else:
                src_y, dst_y, size = ey - ypad, 0, ypad
            if kind == "z":
                src = z_send.at[:, pl.ds(src_y, size)]
                dst = z_recv.at[1 - zs, :, pl.ds(dst_y, size)]
            else:
                src = xz_send.at[xs, pl.ds(src_y, size)]
                dst = xz_recv.at[1 - xs, 1 - zs, pl.ds(dst_y, size)]
        copy = pltpu.make_async_remote_copy(
            src_ref=src,
            dst_ref=dst,
            send_sem=send_sem.at[number],
            recv_sem=recv_sem.at[number],
            device_id=target,
            device_id_type=MESH,
        )
        return copy, exists(dx, dy, dz), exists(-dx, -dy, -dz)

    for number in range(len(MESSAGES)):
        copy, to_there, _ = describe(number)

        @pl.when(to_there)
        def _():
            copy.start()

    rounds = []
    radius = reach
    while radius < count_z - 1:
        rounds.append(radius)
        radius *= 2

    def hello(number):
        for side, step in enumerate((-rounds[number], rounds[number])):

            @pl.when(exists(0, 0, step))
            def _():
                pl.semaphore_signal(
                    hello_sem.at[number, 1 - side],
                    inc=1,
                    device_id=(me[0], me[1], me[2] + step),
                    device_id_type=MESH,
                )

    def hear(number):
        for side, step in enumerate((-rounds[number], rounds[number])):

            @pl.when(exists(0, 0, step))
            def _():
                pl.semaphore_wait(hello_sem.at[number, side], 1)

    if rounds:
        hello(0)

    def wait_for(part, send):
        for number, message in enumerate(MESSAGES):
            far = message[0] in ("y", "xy") and message[4] == 1
            if send and (message[0] == "x") != (part == 0):
                continue
            if not send and far != (part == 1):
                continue
            copy, to_there, from_there = describe(number)

            @pl.when(to_there if send else from_there)
            def _():
                if send:
                    copy.wait_send()
                else:
                    copy.wait_recv()

    def unpack_y(part):
        for side in range(2):
            for layer in range(2):
                y = (
                    ypad - 2 - 2 * part + layer
                    if side == 0
                    else ypad + ey + 2 * part + layer
                )
                for f in range(4):
                    for half in range(ex // 8):
                        base[
                            0, f, pl.ds((HALO + 8 * half) * rows + y, 8, stride=rows)
                        ] = y_recv[side, part, f, layer, pl.ds(8 * half, 8)]
                    for xs in range(2):
                        x0 = 0 if xs == 0 else HALO + ex
                        base[0, f, pl.ds(x0 * rows + y, HALO, stride=rows)] = xy_recv[
                            xs, side, part, f, layer
                        ]

    def unpack_z():
        lane_rows = lax.broadcasted_iota(jnp.int32, (rows, LANES), 1)
        lower = lax.rem(lane_rows, 8) < HALO
        for f in range(4):
            merged = jnp.where(lower, z_recv[0, f], z_recv[1, f])
            for k in range(ex):
                base[1, f, pl.ds((HALO + k) * rows, rows)] = pltpu.roll(
                    merged, (2 * LANES - 8 * k - HALO) % LANES, 1
                )
        for xs in range(2):
            merged = jnp.where(lower, xz_recv[xs, 0], xz_recv[xs, 1])
            for f in range(4):
                for j in range(HALO):
                    k = f * HALO + j
                    x = j if xs == 0 else HALO + ex + j
                    base[1, f, pl.ds(x * rows, rows)] = pltpu.roll(
                        merged, (2 * LANES - 8 * k - HALO) % LANES, 1
                    )

    lane = lax.broadcasted_iota(jnp.int32, (wide_y, LANES), 1)
    row_y = lax.broadcasted_iota(jnp.int32, (wide_y, LANES), 0)
    at_y = me[1] * ey + row_y - HALO
    good_y = (at_y >= 0) & (at_y < ey * count_y)
    good_halo = (
        good_y
        & ((me[2] > 0) | (lane < LANES // 2))
        & ((me[2] < count_z - 1) | (lane >= LANES // 2))
    )
    goods = (good_y, good_halo)

    def at(x, dy=0, own=False):
        if own:
            return pl.ds(x * rows + ypad + dy, ey)
        return pl.ds(x * rows + first_y + dy, wide_y)

    def prepare(x, carry):
        at_x = me[0] * ex + x - HALO
        good_x = (at_x >= 0) & (at_x < ex * count_x)
        for t in range(2):
            good = goods[t] & good_x
            g = jnp.where(good, base[t, 3, at(x)], 1.0)
            base[t, 3, at(x)] = g
            inv = jnp.where(good, RELAXATION / (g * DIAGONAL + MASS_TERM), 0.0)
            inverse[t, at(x)] = inv
            for c in range(3):
                load = jnp.where(good, base[t, c, at(x)], 0.0)
                base[t, c, at(x)] = load
                field_a[t, c, at(x)] = load * inv
        return carry

    def image(field, x, own=False):
        parts = [[None] * 3, [None] * 3]
        ups = [[None] * 3, [None] * 3]
        downs = [[None] * 3, [None] * 3]
        for t in range(2):

            def load(c, ox, oy):
                return field[t, c, at(x + ox, oy, own)]

            centre = [load(c, 0, 0) for c in range(3)]
            x_up = [load(c, 1, 0) for c in range(3)]
            x_down = [load(c, -1, 0) for c in range(3)]
            y_up = [load(c, 0, 1) for c in range(3)]
            y_down = [load(c, 0, -1) for c in range(3)]

            def corners(c):
                return (load(c, 1, 1) - load(c, 1, -1)) - (load(c, -1, 1) - load(c, -1, -1))

            sum_x = [x_up[c] + x_down[c] for c in range(3)]
            sum_y = [y_up[c] + y_down[c] for c in range(3)]
            parts[t][0] = DIAGONAL * centre[0] - OWN * sum_x[0] - sum_y[0] - CROSS * corners(1)
            parts[t][1] = DIAGONAL * centre[1] - sum_x[1] - OWN * sum_y[1] - CROSS * corners(0)
            parts[t][2] = DIAGONAL * centre[2] - sum_x[2] - sum_y[2]
            tilt_x = CROSS * (x_up[2] - x_down[2])
            tilt_y = CROSS * (y_up[2] - y_down[2])
            tilt_z = CROSS * ((x_up[0] - x_down[0]) + (y_up[1] - y_down[1]))
            own_z = OWN * centre[2]
            ups[t] = [centre[0] + tilt_x, centre[1] + tilt_y, own_z + tilt_z]
            downs[t] = [centre[0] - tilt_x, centre[1] - tilt_y, own_z - tilt_z]
        out = [[None] * 3, [None] * 3]
        lanes = lax.broadcasted_iota(jnp.int32, parts[0][0].shape, 1)
        first_lane = lanes == 0
        last_lane = lanes == LANES - 1
        for c in range(3):
            up = [pltpu.roll(ups[t][c], LANES - 1, 1) for t in range(2)]
            down = [pltpu.roll(downs[t][c], 1, 1) for t in range(2)]
            for t in range(2):
                beside = jnp.where(last_lane, up[1 - t], up[t]) + jnp.where(
                    first_lane, down[1 - t], down[t]
                )
                out[t][c] = parts[t][c] - beside
        return out

    def residual(field, x, tiles, own=False):
        images = image(field, x, own)
        out = []
        here = at(x, 0, own)
        for t in tiles:
            g = base[t, 3, here]
            out.append(
                [
                    base[t, c, here] - (g * images[t][c] + MASS_TERM * field[t, c, here])
                    for c in range(3)
                ]
            )
        return out

    def sweep(source, target, low, high):
        def one(x, carry):
            left = residual(source, x, (0, 1))
            for t in range(2):
                inv = inverse[t, at(x)]
                for c in range(3):
                    target[t, c, at(x)] = source[t, c, at(x)] + inv * left[t][c]
            return carry

        lax.fori_loop(low, high, one, 0)

    def fold(value):
        return jnp.sum(value.reshape(ey // 8, 8, LANES), axis=0)

    zero = jnp.zeros((8, LANES), jnp.float32)

    wait_for(0, False)
    wait_for(0, True)
    unpack_y(0)
    unpack_z()
    lax.fori_loop(2, wide_x - 2, prepare, 0)
    sweep(field_a, field_b, 3, wide_x - 3)

    def restrict(x, carry):
        left = residual(field_b, x, (0,), True)[0]
        sums = [carry[c] + fold(left[c]) for c in range(3)]
        sums.append(carry[3] + fold(base[0, 3, at(x, 0, True)]))
        return tuple(sums)

    sums = lax.fori_loop(HALO, HALO + ex, restrict, (zero,) * 4)
    stacked = jnp.concatenate([jnp.sum(s, axis=0, keepdims=True) for s in sums] + [zero[:4]], axis=0)
    source_lane = lax.broadcasted_iota(jnp.int32, (LANES, LANES), 0)
    target_lane = lax.broadcasted_iota(jnp.int32, (LANES, LANES), 1)
    gather = (source_lane // BLOCK == lax.rem(target_lane, cz)).astype(jnp.float32)
    grouped = jnp.dot(stacked, gather, precision=EXACT, preferred_element_type=jnp.float32)
    coarse_send[...] = grouped[:4]

    def coarse_copy(x, y, z, dz):
        return pltpu.make_async_remote_copy(
            src_ref=coarse_send,
            dst_ref=coarse_recv.at[reach - dz, me[0], me[1]],
            send_sem=coarse_send_sem.at[reach + dz, x, y],
            recv_sem=coarse_recv_sem.at[reach - dz, me[0], me[1]],
            device_id=(x, y, z),
            device_id_type=MESH,
        )

    def coarse_wait(x, y, z, dz):
        pltpu.make_async_remote_copy(
            src_ref=coarse_send,
            dst_ref=coarse_recv.at[reach + dz, x, y],
            send_sem=coarse_send_sem.at[reach + dz, x, y],
            recv_sem=coarse_recv_sem.at[reach + dz, x, y],
            device_id=(x, y, z),
            device_id_type=MESH,
        ).wait()

    peers(lambda x, y, z, dz: coarse_copy(x, y, z, dz).start())
    coarse_recv[reach, me[0], me[1]] = grouped[:4]

    wait_for(1, False)
    unpack_y(1)
    lax.fori_loop(0, wide_x, prepare, 0)
    sweep(field_a, field_b, 1, wide_x - 1)
    sweep(field_b, field_a, 2, wide_x - 2)

    def load_squares(x, carry):
        loads = [base[0, c, at(x, 0, True)] for c in range(3)]
        return carry + fold(sum(value * value for value in loads))

    load_sum = lax.fori_loop(HALO, HALO + ex, load_squares, zero)
    wait_for(1, True)
    for number in range(len(rounds)):
        if number > 0:
            hello(number)
        hear(number)
    peers(coarse_wait)

    coarse_rows = -(-(count_y + 1) // 8) * 8
    lane_c = lax.broadcasted_iota(jnp.int32, (coarse_rows, LANES), 1)
    row_c = lax.broadcasted_iota(jnp.int32, (coarse_rows, LANES), 0)
    at_z = me[2] * cz - reach * cz + lane_c
    valid = (
        (row_c < count_y) & (at_z >= 0) & (at_z < cz * count_z) & (lane_c < window * cz)
    )
    slab = [[None] * 4 for _ in range(count_x)]
    for x in range(count_x):
        for c in range(4):
            value = None
            for w in range(window):
                column = jnp.concatenate(
                    [coarse_recv[w, x, y, c : c + 1] for y in range(count_y)]
                    + [jnp.zeros((coarse_rows - count_y, LANES), jnp.float32)],
                    axis=0,
                )
                value = column if value is None else jnp.where(lane_c // cz == w, column, value)
            slab[x][c] = jnp.where(valid, value, 0.0)
    mass = BLOCK**3 * MASS_TERM
    factor = [slab[x][3] * (BLOCK**2 / BLOCK**3) for x in range(count_x)]
    relax = [
        jnp.where(valid, RELAXATION / (factor[x] * DIAGONAL + mass), 0.0) for x in range(count_x)
    ]
    nothing = jnp.zeros((coarse_rows, LANES), jnp.float32)
    w = [[slab[x][c] * relax[x] for c in range(3)] for x in range(count_x)]

    def y_shift(value, step):
        return pltpu.roll(value, step % coarse_rows, 0)

    def z_shift(value, step):
        return pltpu.roll(value, step % LANES, 1)

    for repeat in range(COARSE - 1):
        fresh = []
        for x in range(count_x):
            here = w[x]
            above = w[x + 1] if x + 1 < count_x else [nothing] * 3
            below = w[x - 1] if x > 0 else [nothing] * 3
            sum_x = [above[c] + below[c] for c in range(3)]
            diff_x = [above[c] - below[c] for c in range(3)]
            y_up = [y_shift(here[c], -1) for c in range(3)]
            y_down = [y_shift(here[c], 1) for c in range(3)]
            sum_y = [y_up[c] + y_down[c] for c in range(3)]
            diff_y = [y_up[c] - y_down[c] for c in range(3)]
            corner_x = y_shift(diff_x[1], -1) - y_shift(diff_x[1], 1)
            corner_y = y_shift(diff_x[0], -1) - y_shift(diff_x[0], 1)
            tilt = [CROSS * diff_x[2], CROSS * diff_y[2], CROSS * (diff_x[0] + diff_y[1])]
            own = [here[0], here[1], OWN * here[2]]
            beside = [z_shift(own[c] + tilt[c], -1) + z_shift(own[c] - tilt[c], 1) for c in range(3)]
            flat = [
                DIAGONAL * here[0] - OWN * sum_x[0] - sum_y[0] - CROSS * corner_x - beside[0],
                DIAGONAL * here[1] - sum_x[1] - OWN * sum_y[1] - CROSS * corner_y - beside[1],
                DIAGONAL * here[2] - sum_x[2] - sum_y[2] - beside[2],
            ]
            fresh.append(
                [
                    here[c] + relax[x] * (slab[x][c] - (factor[x] * flat[c] + mass * here[c]))
                    for c in range(3)
                ]
            )
        w = fresh

    for x in range(count_x + 2):
        for c in range(3):
            inside = 1 <= x <= count_x
            coarse_w[x, c, pl.ds(0, 8)] = jnp.zeros((8, LANES), jnp.float32)
            coarse_w[x, c, pl.ds(8, coarse_rows)] = w[x - 1][c] if inside else nothing
    widen_core = (source_lane == reach * cz + target_lane // BLOCK).astype(jnp.float32)
    widen_halo = (
        source_lane == jnp.where(target_lane < LANES // 2, (reach + 1) * cz, reach * cz - 1)
    ).astype(jnp.float32)
    for xc in range(3):
        for c in range(3):
            cells = [coarse_w[me[0] + xc, c, pl.ds(7 + me[1] + k, 1)] for k in range(3)]
            stacked = jnp.concatenate(cells + [zero[:5]], axis=0)
            for t, matrix in enumerate((widen_core, widen_halo)):
                wide = jnp.dot(stacked, matrix, precision=EXACT, preferred_element_type=jnp.float32)
                low = jnp.broadcast_to(wide[0:1], (wide_y, LANES))
                mid = jnp.broadcast_to(wide[1:2], (wide_y, LANES))
                top = jnp.broadcast_to(wide[2:3], (wide_y, LANES))
                wide = jnp.where(row_y < HALO, low, jnp.where(row_y < HALO + ey, mid, top))
                for plane in range(3):
                    spread_w[t, c, pl.ds((3 * xc + plane) * rows + first_y, wide_y)] = wide
    for plane in range(1, 8):
        images = image(spread_w, plane)
        for t in range(2):
            for c in range(3):
                image_w[t, c, at(plane)] = images[t][c]

    def correct(x, carry):
        kind = (
            1
            + (x >= HALO - 1).astype(jnp.int32)
            + (x >= HALO).astype(jnp.int32)
            + (x >= HALO + 1).astype(jnp.int32)
            + (x >= HALO + ex - 1).astype(jnp.int32)
            + (x >= HALO + ex).astype(jnp.int32)
            + (x >= HALO + ex + 1).astype(jnp.int32)
        )
        for t in range(2):
            inv = inverse[t, at(x)]
            g = base[t, 3, at(x)]
            for c in range(3):
                added = spread_w[t, c, at(kind)]
                field_a[t, c, at(x)] = (
                    field_a[t, c, at(x)]
                    + added
                    - inv * (g * image_w[t, c, at(kind)] + MASS_TERM * added)
                )
        return carry

    lax.fori_loop(2, wide_x - 2, correct, 0)
    sweep(field_a, field_b, 3, wide_x - 3)

    def squares(x, carry):
        left = residual(field_b, x, (0,), True)[0]
        for c in range(3):
            out_ref[c, x - HALO] = field_b[0, c, at(x, 0, True)]
        return carry + fold(sum(value * value for value in left))

    left_sum = lax.fori_loop(HALO, HALO + ex, squares, zero)
    load_total = jnp.sum(jnp.sum(load_sum, axis=0, keepdims=True), axis=1, keepdims=True)
    left_total = jnp.sum(jnp.sum(left_sum, axis=0, keepdims=True), axis=1, keepdims=True)
    first = lax.broadcasted_iota(jnp.int32, (1, LANES), 1) == 0
    mine = jnp.where(first, load_total, left_total)
    norm_send[...] = mine

    def norm_copy(step):
        return pltpu.make_async_remote_copy(
            src_ref=norm_send,
            dst_ref=norm_recv.at[step - 1],
            send_sem=norm_send_sem.at[step - 1],
            recv_sem=norm_recv_sem.at[step - 1],
            device_id=place(lax.rem(my_id + step, total)),
            device_id_type=MESH,
        )

    def norm_start(step, carry):
        norm_copy(step).start()
        return carry

    def norm_wait(step, carry):
        norm_copy(step).wait()
        return carry

    lax.fori_loop(1, total, norm_start, 0)
    norm_recv[total - 1] = mine
    lax.fori_loop(1, total, norm_wait, 0)

    def add(device, carry):
        slot = lax.rem(my_id - device + total - 1, total)
        return carry + norm_recv[lax.rem(slot + total, total)]

    summed = lax.fori_loop(0, total, add, jnp.zeros((1, LANES), jnp.float32))
    nodes = 3 * ex * ey * ez * total
    norms_ref[...] = jnp.sqrt(summed / nodes)


def on_device(counts, right_side, damage):
    _, ex, ey, ez = right_side.shape
    cz = ez // BLOCK
    wide_x = ex + 2 * HALO
    rows = ey + 16
    flat = wide_x * rows
    wide_y = ey + 2 * HALO
    total = counts[0] * counts[1] * counts[2]
    window = 2 * (-(-COARSE // cz)) + 1
    coarse_rows = -(-(counts[1] + 1) // 8) * 8
    f32 = jnp.float32
    vmem = pltpu.VMEM
    dma = pltpu.SemaphoreType.DMA
    displacement, norms = pl.pallas_call(
        functools.partial(kernel, counts, (ex, ey, ez)),
        out_shape=(
            pltpu.VMEM(right_side.shape, f32),
            pltpu.VMEM((1, LANES), f32),
        ),
        in_specs=[pl.BlockSpec(memory_space=pl.ANY)] * 2,
        out_specs=(
            pl.BlockSpec(memory_space=pltpu.VMEM),
            pl.BlockSpec(memory_space=pltpu.VMEM),
        ),
        scratch_shapes=[
            vmem((2, 4, flat, LANES), f32),
            vmem((2, flat, LANES), f32),
            vmem((2, 3, flat, LANES), f32),
            vmem((2, 3, flat, LANES), f32),
            vmem((ex, ey, LANES), jnp.int32),
            vmem((2, 2, 4, 2, ex, LANES), f32),
            vmem((2, 2, 4, 2, ex, LANES), f32),
            vmem((2, 2, 2, 4, 2, HALO, LANES), f32),
            vmem((2, 2, 2, 4, 2, HALO, LANES), f32),
            vmem((4, ey, LANES), f32),
            vmem((2, 4, rows, LANES), f32),
            vmem((2, ey, LANES), f32),
            vmem((2, 2, rows, LANES), f32),
            vmem((4, LANES), f32),
            vmem((window, counts[0], counts[1], 4, LANES), f32),
            vmem((counts[0] + 2, 3, 8 + coarse_rows, LANES), f32),
            vmem((2, 3, 9 * rows, LANES), f32),
            vmem((2, 3, 9 * rows, LANES), f32),
            vmem((1, LANES), f32),
            vmem((total, 1, LANES), f32),
            dma((ex + 1,)),
            dma((len(MESSAGES),)),
            dma((len(MESSAGES),)),
            dma((window, counts[0], counts[1])),
            dma((window, counts[0], counts[1])),
            dma((total,)),
            dma((total,)),
            pltpu.SemaphoreType.REGULAR((8, 2)),
        ],
        compiler_params=pltpu.CompilerParams(collective_id=0, has_side_effects=True),
    )(right_side, damage)
    return displacement, norms[0, :2]


def solution(mesh):
    counts = tuple(mesh.shape[axis] for axis in AXES)
    placed = (P(None, "gx", "gy", "gz"), P("gx", "gy", "gz"))
    return jax.shard_map(
        functools.partial(on_device, counts),
        mesh=mesh,
        in_specs=placed,
        out_specs=(P(None, "gx", "gy", "gz"), P()),
        check_vma=False,
    )
```

```python
import functools

import jax
import jax.numpy as jnp
from jax import lax
from jax.experimental import pallas as pl
from jax.experimental.pallas import tpu as pltpu
from jax.sharding import PartitionSpec as P

BLOCK = 16
COARSE = 8
FLOOR_STIFFNESS = 0.05
MASS_TERM = 0.001
COUPLING = 2.5
RELAXATION = 0.6
DIAGONAL = 6.0 + 2.0 * COUPLING
OWN = 1.0 + COUPLING
CROSS = 0.25 * COUPLING
AXES = ("gx", "gy", "gz")
HALO = 4
LANES = 128
MESH = pl.DeviceIdType.MESH
EXACT = lax.Precision.HIGHEST


def messages():
    out = []
    for dx in (-1, 1):
        for part in range(HALO):
            out.append(("x", dx, 0, 0, part))
    for part in range(2):
        for dy in (-1, 1):
            out.append(("y", 0, dy, 0, part))
        for dx in (-1, 1):
            for dy in (-1, 1):
                if part == 1:
                    out.append(("xy", dx, dy, 0, part))
                out.append(("xyn", dx, dy, 0, part))
        if part == 0:
            for dz in (-1, 1):
                for dx in (-1, 0, 1):
                    for dy in (-1, 0, 1):
                        out.append(("z" if dx == 0 else "xz", dx, dy, dz, 0))
    return out


MESSAGES = messages()


def kernel(
    counts,
    extent,
    load_ref,
    damage_ref,
    out_ref,
    norms_ref,
    base,
    inverse,
    field_a,
    field_b,
    harm,
    y_send,
    y_recv,
    xy_send,
    xy_recv,
    xyn_send,
    xyn_recv,
    yz_send,
    yz_recv,
    xyz_send,
    xyz_recv,
    z_send,
    z_recv,
    xz_send,
    xz_recv,
    coarse_send,
    coarse_recv,
    coarse_w,
    spread_w,
    image_w,
    norm_send,
    norm_recv,
    local_sem,
    send_sem,
    recv_sem,
    coarse_send_sem,
    coarse_recv_sem,
    norm_send_sem,
    norm_recv_sem,
    hello_sem,
):
    count_x, count_y, count_z = counts
    ex, ey, ez = extent
    cz = ez // BLOCK
    total = count_x * count_y * count_z
    wide_x = ex + 2 * HALO
    ypad = 8
    rows = ey + 2 * ypad
    wide_y = ey + 2 * HALO
    first_y = ypad - HALO
    me = tuple(lax.axis_index(axis) for axis in AXES)
    my_id = (me[0] * count_y + me[1]) * count_z + me[2]

    def place(index):
        return (
            index // (count_y * count_z),
            lax.rem(index // count_z, count_y),
            lax.rem(index, count_z),
        )

    load_copies = []
    for x in range(ex):
        target = pl.ds((HALO + x) * rows + ypad, ey)
        load_copies.append(
            pltpu.make_async_copy(load_ref.at[:, x], base.at[0, 0:3, target], local_sem.at[x])
        )
    harm_copy = pltpu.make_async_copy(damage_ref, harm, local_sem.at[ex])
    harm_copy.start()
    for copy in load_copies:
        copy.start()

    barrier = pltpu.get_barrier_semaphore()

    reach = -(-COARSE // cz)
    window = 2 * reach + 1

    def peers(act):
        for dz in range(-reach, reach + 1):
            z = me[2] + dz

            @pl.when((z >= 0) & (z < count_z))
            def _():
                def one(step, carry):
                    if dz == 0:
                        step = step + 1
                    index = lax.rem(me[0] * count_y + me[1] + step, count_x * count_y)
                    act(index // count_y, lax.rem(index, count_y), z, dz)
                    return carry

                lax.fori_loop(0, count_x * count_y - (1 if dz == 0 else 0), one, 0)

    def greet(x, y, z, dz):
        pl.semaphore_signal(barrier, inc=1, device_id=(x, y, z), device_id_type=MESH)

    peers(greet)
    levels = jnp.minimum(me[2] + reach, count_z - 1) - jnp.maximum(me[2] - reach, 0) + 1

    harm_copy.wait()
    for x in range(ex):
        level = 1.0 - harm[x].astype(jnp.float32) / 15.0
        base[0, 3, pl.ds((HALO + x) * rows + ypad, ey)] = (
            level * level * (1.0 - FLOOR_STIFFNESS) + FLOOR_STIFFNESS
        )
    for copy in load_copies:
        copy.wait()

    lane = lax.broadcasted_iota(jnp.int32, (ey, LANES), 1)
    for side in range(2):
        for part in range(2):
            for layer in range(2):
                y = 2 * part + layer if side == 0 else ey - 2 - 2 * part + layer
                for f in range(4):
                    start = HALO * rows + ypad + y
                    for half in range(ex // 8):
                        y_send[side, part, f, layer, pl.ds(8 * half, 8)] = base[
                            0, f, pl.ds(start + 8 * half * rows, 8, stride=rows)
                        ]
                    for xs in range(2):
                        x0 = 0 if xs == 0 else ex - HALO
                        if part == 1:
                            xy_send[xs, side, f, layer] = base[
                                0, f, pl.ds(start + x0 * rows, HALO, stride=rows)
                            ]
                            continue
                        for which in range(2):
                            x0 = 2 * which if xs == 0 else ex - 2 - 2 * which
                            xyn_send[xs, side, which, f, layer] = base[
                                0, f, pl.ds(start + x0 * rows, 2, stride=rows)
                            ]
    for f in range(4):
        packed = None
        for k in range(ex):
            row = base[0, f, pl.ds((HALO + k) * rows + ypad, ey)]
            moved = pltpu.roll(row, (8 * k + HALO) % LANES, 1)
            packed = moved if packed is None else jnp.where(lane // 8 == k, moved, packed)
        z_send[f] = packed
        yz_send[0, f] = packed[:HALO]
        yz_send[1, f] = packed[ey - HALO :]
    for xs in range(2):
        packed = None
        for f in range(4):
            for j in range(HALO):
                x = j if xs == 0 else ex - HALO + j
                k = f * HALO + j
                row = base[0, f, pl.ds((HALO + x) * rows + ypad, ey)]
                moved = pltpu.roll(row, (8 * k + HALO) % LANES, 1)
                packed = moved if packed is None else jnp.where(lane // 8 == k, moved, packed)
        xz_send[xs] = packed
        xyz_send[xs, 0] = packed[:HALO]
        xyz_send[xs, 1] = packed[ey - HALO :]

    pl.semaphore_wait(barrier, levels * count_x * count_y - 1)

    def exists(dx, dy, dz):
        ok = None
        for axis, step in enumerate((dx, dy, dz)):
            if step == 0:
                continue
            here = me[axis] + step
            good = (here >= 0) & (here < counts[axis])
            ok = good if ok is None else ok & good
        return ok

    def describe(number):
        kind, dx, dy, dz, part = MESSAGES[number]
        target = (me[0] + dx, me[1] + dy, me[2] + dz)
        xs, ys, zs = (dx + 1) // 2, (dy + 1) // 2, (dz + 1) // 2
        if kind == "x":
            src_x = HALO + part if dx < 0 else ex + part
            dst_x = HALO + ex + part if dx < 0 else part
            src = base.at[0, :, pl.ds(src_x * rows + ypad, ey)]
            dst = base.at[0, :, pl.ds(dst_x * rows + ypad, ey)]
        elif kind == "y":
            src, dst = y_send.at[ys, part], y_recv.at[1 - ys, part]
        elif kind == "xy":
            src, dst = xy_send.at[xs, ys], xy_recv.at[1 - xs, 1 - ys]
        elif kind == "xyn":
            src, dst = xyn_send.at[xs, ys, part], xyn_recv.at[1 - xs, 1 - ys, part]
        else:
            own = pl.ds(ypad, ey)
            if kind == "z" and dy == 0:
                src, dst = z_send, z_recv.at[1 - zs, :, own]
            elif kind == "z":
                src, dst = yz_send.at[ys], yz_recv.at[1 - zs, 1 - ys]
            elif dy == 0:
                src, dst = xz_send.at[xs], xz_recv.at[1 - xs, 1 - zs, own]
            else:
                src, dst = xyz_send.at[xs, ys], xyz_recv.at[1 - xs, 1 - zs, 1 - ys]
        copy = pltpu.make_async_remote_copy(
            src_ref=src,
            dst_ref=dst,
            send_sem=send_sem.at[number],
            recv_sem=recv_sem.at[number],
            device_id=target,
            device_id_type=MESH,
        )
        return copy, exists(dx, dy, dz), exists(-dx, -dy, -dz)

    for number in range(len(MESSAGES)):
        copy, to_there, _ = describe(number)

        @pl.when(to_there)
        def _():
            copy.start()

    rounds = []
    radius = reach
    while radius < count_z - 1:
        rounds.append(radius)
        radius *= 2

    def hello(number):
        for side, step in enumerate((-rounds[number], rounds[number])):

            @pl.when(exists(0, 0, step))
            def _():
                pl.semaphore_signal(
                    hello_sem.at[number, 1 - side],
                    inc=1,
                    device_id=(me[0], me[1], me[2] + step),
                    device_id_type=MESH,
                )

    def hear(number):
        for side, step in enumerate((-rounds[number], rounds[number])):

            @pl.when(exists(0, 0, step))
            def _():
                pl.semaphore_wait(hello_sem.at[number, side], 1)

    if rounds:
        hello(0)

    def wait_for(part, send):
        for number, message in enumerate(MESSAGES):
            far = message[0] in ("y", "xy", "xyn") and message[4] == 1
            if send and (message[0] == "x") != (part == 0):
                continue
            if not send and far != (part == 1):
                continue
            copy, to_there, from_there = describe(number)

            @pl.when(to_there if send else from_there)
            def _():
                if send:
                    copy.wait_send()
                else:
                    copy.wait_recv()

    def unpack_y(part):
        for side in range(2):
            for layer in range(2):
                y = (
                    ypad - 2 - 2 * part + layer
                    if side == 0
                    else ypad + ey + 2 * part + layer
                )
                for f in range(4):
                    for half in range(ex // 8):
                        base[
                            0, f, pl.ds((HALO + 8 * half) * rows + y, 8, stride=rows)
                        ] = y_recv[side, part, f, layer, pl.ds(8 * half, 8)]
                    near_y = ypad - 2 + layer if side == 0 else ypad + ey + layer
                    for xs in range(2):
                        x0 = 0 if xs == 0 else HALO + ex
                        if part == 1:
                            base[0, f, pl.ds(x0 * rows + y, HALO, stride=rows)] = xy_recv[
                                xs, side, f, layer
                            ]
                        x0 = 2 - 2 * part if xs == 0 else HALO + ex + 2 * part
                        base[0, f, pl.ds(x0 * rows + near_y, 2, stride=rows)] = xyn_recv[
                            xs, side, part, f, layer
                        ]

    def unpack_z():
        lane_rows = lax.broadcasted_iota(jnp.int32, (rows, LANES), 1)
        lower = lax.rem(lane_rows, 8) < HALO
        for zs in range(2):
            for ys in range(2):
                edge = pl.ds(first_y if ys == 0 else ypad + ey, HALO)
                for f in range(4):
                    z_recv[zs, f, edge] = yz_recv[zs, ys, f]
                for xs in range(2):
                    xz_recv[xs, zs, edge] = xyz_recv[xs, zs, ys]
        for f in range(4):
            merged = jnp.where(lower, z_recv[0, f], z_recv[1, f])
            for k in range(ex):
                base[1, f, pl.ds((HALO + k) * rows, rows)] = pltpu.roll(
                    merged, (2 * LANES - 8 * k - HALO) % LANES, 1
                )
        for xs in range(2):
            merged = jnp.where(lower, xz_recv[xs, 0], xz_recv[xs, 1])
            for f in range(4):
                for j in range(HALO):
                    k = f * HALO + j
                    x = j if xs == 0 else HALO + ex + j
                    base[1, f, pl.ds(x * rows, rows)] = pltpu.roll(
                        merged, (2 * LANES - 8 * k - HALO) % LANES, 1
                    )

    lane = lax.broadcasted_iota(jnp.int32, (wide_y, LANES), 1)
    row_y = lax.broadcasted_iota(jnp.int32, (wide_y, LANES), 0)
    at_y = me[1] * ey + row_y - HALO
    good_y = (at_y >= 0) & (at_y < ey * count_y)
    good_halo = (
        good_y
        & ((me[2] > 0) | (lane < LANES // 2))
        & ((me[2] < count_z - 1) | (lane >= LANES // 2))
    )
    goods = (good_y, good_halo)

    def at(x, dy=0, own=False):
        if own:
            return pl.ds(x * rows + ypad + dy, ey)
        return pl.ds(x * rows + first_y + dy, wide_y)

    def prepare(x, carry):
        at_x = me[0] * ex + x - HALO
        good_x = (at_x >= 0) & (at_x < ex * count_x)
        for t in range(2):
            good = goods[t] & good_x
            g = jnp.where(good, base[t, 3, at(x)], 1.0)
            base[t, 3, at(x)] = g
            inv = jnp.where(good, RELAXATION / (g * DIAGONAL + MASS_TERM), 0.0)
            inverse[t, at(x)] = inv
            for c in range(3):
                load = jnp.where(good, base[t, c, at(x)], 0.0)
                base[t, c, at(x)] = load
                field_a[t, c, at(x)] = load * inv
        return carry

    def image(field, x, own=False):
        parts = [[None] * 3, [None] * 3]
        ups = [[None] * 3, [None] * 3]
        downs = [[None] * 3, [None] * 3]
        for t in range(2):

            def load(c, ox, oy):
                return field[t, c, at(x + ox, oy, own)]

            centre = [load(c, 0, 0) for c in range(3)]
            x_up = [load(c, 1, 0) for c in range(3)]
            x_down = [load(c, -1, 0) for c in range(3)]
            y_up = [load(c, 0, 1) for c in range(3)]
            y_down = [load(c, 0, -1) for c in range(3)]

            def corners(c):
                return (load(c, 1, 1) - load(c, 1, -1)) - (load(c, -1, 1) - load(c, -1, -1))

            sum_x = [x_up[c] + x_down[c] for c in range(3)]
            sum_y = [y_up[c] + y_down[c] for c in range(3)]
            parts[t][0] = DIAGONAL * centre[0] - OWN * sum_x[0] - sum_y[0] - CROSS * corners(1)
            parts[t][1] = DIAGONAL * centre[1] - sum_x[1] - OWN * sum_y[1] - CROSS * corners(0)
            parts[t][2] = DIAGONAL * centre[2] - sum_x[2] - sum_y[2]
            tilt_x = CROSS * (x_up[2] - x_down[2])
            tilt_y = CROSS * (y_up[2] - y_down[2])
            tilt_z = CROSS * ((x_up[0] - x_down[0]) + (y_up[1] - y_down[1]))
            own_z = OWN * centre[2]
            ups[t] = [centre[0] + tilt_x, centre[1] + tilt_y, own_z + tilt_z]
            downs[t] = [centre[0] - tilt_x, centre[1] - tilt_y, own_z - tilt_z]
        out = [[None] * 3, [None] * 3]
        lanes = lax.broadcasted_iota(jnp.int32, parts[0][0].shape, 1)
        first_lane = lanes == 0
        last_lane = lanes == LANES - 1
        for c in range(3):
            up = [pltpu.roll(ups[t][c], LANES - 1, 1) for t in range(2)]
            down = [pltpu.roll(downs[t][c], 1, 1) for t in range(2)]
            for t in range(2):
                beside = jnp.where(last_lane, up[1 - t], up[t]) + jnp.where(
                    first_lane, down[1 - t], down[t]
                )
                out[t][c] = parts[t][c] - beside
        return out

    def residual(field, x, tiles, own=False):
        images = image(field, x, own)
        out = []
        here = at(x, 0, own)
        for t in tiles:
            g = base[t, 3, here]
            out.append(
                [
                    base[t, c, here] - (g * images[t][c] + MASS_TERM * field[t, c, here])
                    for c in range(3)
                ]
            )
        return out

    def sweep(source, target, low, high):
        def one(x, carry):
            left = residual(source, x, (0, 1))
            for t in range(2):
                inv = inverse[t, at(x)]
                for c in range(3):
                    target[t, c, at(x)] = source[t, c, at(x)] + inv * left[t][c]
            return carry

        lax.fori_loop(low, high, one, 0)

    def fold(value):
        return jnp.sum(value.reshape(ey // 8, 8, LANES), axis=0)

    zero = jnp.zeros((8, LANES), jnp.float32)

    wait_for(0, False)
    wait_for(0, True)
    unpack_y(0)
    unpack_z()
    lax.fori_loop(2, wide_x - 2, prepare, 0)
    sweep(field_a, field_b, 3, wide_x - 3)

    def restrict(x, carry):
        left = residual(field_b, x, (0,), True)[0]
        sums = [carry[c] + fold(left[c]) for c in range(3)]
        sums.append(carry[3] + fold(base[0, 3, at(x, 0, True)]))
        return tuple(sums)

    sums = lax.fori_loop(HALO, HALO + ex, restrict, (zero,) * 4)
    stacked = jnp.concatenate([jnp.sum(s, axis=0, keepdims=True) for s in sums] + [zero[:4]], axis=0)
    source_lane = lax.broadcasted_iota(jnp.int32, (LANES, LANES), 0)
    target_lane = lax.broadcasted_iota(jnp.int32, (LANES, LANES), 1)
    gather = (source_lane // BLOCK == lax.rem(target_lane, cz)).astype(jnp.float32)
    grouped = jnp.dot(stacked, gather, precision=EXACT, preferred_element_type=jnp.float32)
    coarse_send[...] = grouped[:4]

    def coarse_copy(x, y, z, dz):
        return pltpu.make_async_remote_copy(
            src_ref=coarse_send,
            dst_ref=coarse_recv.at[reach - dz, me[0], me[1]],
            send_sem=coarse_send_sem.at[reach + dz, x, y],
            recv_sem=coarse_recv_sem.at[reach - dz, me[0], me[1]],
            device_id=(x, y, z),
            device_id_type=MESH,
        )

    def coarse_wait(x, y, z, dz):
        pltpu.make_async_remote_copy(
            src_ref=coarse_send,
            dst_ref=coarse_recv.at[reach + dz, x, y],
            send_sem=coarse_send_sem.at[reach + dz, x, y],
            recv_sem=coarse_recv_sem.at[reach + dz, x, y],
            device_id=(x, y, z),
            device_id_type=MESH,
        ).wait()

    peers(lambda x, y, z, dz: coarse_copy(x, y, z, dz).start())
    coarse_recv[reach, me[0], me[1]] = grouped[:4]

    wait_for(1, False)
    unpack_y(1)
    lax.fori_loop(0, wide_x, prepare, 0)
    sweep(field_a, field_b, 1, wide_x - 1)
    sweep(field_b, field_a, 2, wide_x - 2)

    def load_squares(x, carry):
        loads = [base[0, c, at(x, 0, True)] for c in range(3)]
        return carry + fold(sum(value * value for value in loads))

    load_sum = lax.fori_loop(HALO, HALO + ex, load_squares, zero)
    wait_for(1, True)
    for number in range(len(rounds)):
        if number > 0:
            hello(number)
        hear(number)
    peers(coarse_wait)

    coarse_rows = -(-(count_y + 1) // 8) * 8
    lane_c = lax.broadcasted_iota(jnp.int32, (coarse_rows, LANES), 1)
    row_c = lax.broadcasted_iota(jnp.int32, (coarse_rows, LANES), 0)
    at_z = me[2] * cz - reach * cz + lane_c
    valid = (
        (row_c < count_y) & (at_z >= 0) & (at_z < cz * count_z) & (lane_c < window * cz)
    )
    slab = [[None] * 4 for _ in range(count_x)]
    for x in range(count_x):
        for c in range(4):
            value = None
            for w in range(window):
                column = jnp.concatenate(
                    [coarse_recv[w, x, y, c : c + 1] for y in range(count_y)]
                    + [jnp.zeros((coarse_rows - count_y, LANES), jnp.float32)],
                    axis=0,
                )
                value = column if value is None else jnp.where(lane_c // cz == w, column, value)
            slab[x][c] = jnp.where(valid, value, 0.0)
    mass = BLOCK**3 * MASS_TERM
    factor = [slab[x][3] * (BLOCK**2 / BLOCK**3) for x in range(count_x)]
    relax = [
        jnp.where(valid, RELAXATION / (factor[x] * DIAGONAL + mass), 0.0) for x in range(count_x)
    ]
    nothing = jnp.zeros((coarse_rows, LANES), jnp.float32)
    w = [[slab[x][c] * relax[x] for c in range(3)] for x in range(count_x)]

    def y_shift(value, step):
        return pltpu.roll(value, step % coarse_rows, 0)

    def z_shift(value, step):
        return pltpu.roll(value, step % LANES, 1)

    for repeat in range(COARSE - 1):
        fresh = []
        for x in range(count_x):
            here = w[x]
            above = w[x + 1] if x + 1 < count_x else [nothing] * 3
            below = w[x - 1] if x > 0 else [nothing] * 3
            sum_x = [above[c] + below[c] for c in range(3)]
            diff_x = [above[c] - below[c] for c in range(3)]
            y_up = [y_shift(here[c], -1) for c in range(3)]
            y_down = [y_shift(here[c], 1) for c in range(3)]
            sum_y = [y_up[c] + y_down[c] for c in range(3)]
            diff_y = [y_up[c] - y_down[c] for c in range(3)]
            corner_x = y_shift(diff_x[1], -1) - y_shift(diff_x[1], 1)
            corner_y = y_shift(diff_x[0], -1) - y_shift(diff_x[0], 1)
            tilt = [CROSS * diff_x[2], CROSS * diff_y[2], CROSS * (diff_x[0] + diff_y[1])]
            own = [here[0], here[1], OWN * here[2]]
            beside = [z_shift(own[c] + tilt[c], -1) + z_shift(own[c] - tilt[c], 1) for c in range(3)]
            flat = [
                DIAGONAL * here[0] - OWN * sum_x[0] - sum_y[0] - CROSS * corner_x - beside[0],
                DIAGONAL * here[1] - sum_x[1] - OWN * sum_y[1] - CROSS * corner_y - beside[1],
                DIAGONAL * here[2] - sum_x[2] - sum_y[2] - beside[2],
            ]
            fresh.append(
                [
                    here[c] + relax[x] * (slab[x][c] - (factor[x] * flat[c] + mass * here[c]))
                    for c in range(3)
                ]
            )
        w = fresh

    for x in range(count_x + 2):
        for c in range(3):
            inside = 1 <= x <= count_x
            coarse_w[x, c, pl.ds(0, 8)] = jnp.zeros((8, LANES), jnp.float32)
            coarse_w[x, c, pl.ds(8, coarse_rows)] = w[x - 1][c] if inside else nothing
    widen_core = (source_lane == reach * cz + target_lane // BLOCK).astype(jnp.float32)
    widen_halo = (
        source_lane == jnp.where(target_lane < LANES // 2, (reach + 1) * cz, reach * cz - 1)
    ).astype(jnp.float32)
    for xc in range(3):
        for c in range(3):
            cells = [coarse_w[me[0] + xc, c, pl.ds(7 + me[1] + k, 1)] for k in range(3)]
            stacked = jnp.concatenate(cells + [zero[:5]], axis=0)
            for t, matrix in enumerate((widen_core, widen_halo)):
                wide = jnp.dot(stacked, matrix, precision=EXACT, preferred_element_type=jnp.float32)
                low = jnp.broadcast_to(wide[0:1], (wide_y, LANES))
                mid = jnp.broadcast_to(wide[1:2], (wide_y, LANES))
                top = jnp.broadcast_to(wide[2:3], (wide_y, LANES))
                wide = jnp.where(row_y < HALO, low, jnp.where(row_y < HALO + ey, mid, top))
                for plane in range(3):
                    spread_w[t, c, pl.ds((3 * xc + plane) * rows + first_y, wide_y)] = wide
    for plane in range(1, 8):
        images = image(spread_w, plane)
        for t in range(2):
            for c in range(3):
                image_w[t, c, at(plane)] = images[t][c]

    def correct(x, carry):
        kind = (
            1
            + (x >= HALO - 1).astype(jnp.int32)
            + (x >= HALO).astype(jnp.int32)
            + (x >= HALO + 1).astype(jnp.int32)
            + (x >= HALO + ex - 1).astype(jnp.int32)
            + (x >= HALO + ex).astype(jnp.int32)
            + (x >= HALO + ex + 1).astype(jnp.int32)
        )
        for t in range(2):
            inv = inverse[t, at(x)]
            g = base[t, 3, at(x)]
            for c in range(3):
                added = spread_w[t, c, at(kind)]
                field_a[t, c, at(x)] = (
                    field_a[t, c, at(x)]
                    + added
                    - inv * (g * image_w[t, c, at(kind)] + MASS_TERM * added)
                )
        return carry

    lax.fori_loop(2, wide_x - 2, correct, 0)
    sweep(field_a, field_b, 3, wide_x - 3)

    def squares(x, carry):
        left = residual(field_b, x, (0,), True)[0]
        for c in range(3):
            out_ref[c, x - HALO] = field_b[0, c, at(x, 0, True)]
        return carry + fold(sum(value * value for value in left))

    left_sum = lax.fori_loop(HALO, HALO + ex, squares, zero)
    load_total = jnp.sum(jnp.sum(load_sum, axis=0, keepdims=True), axis=1, keepdims=True)
    left_total = jnp.sum(jnp.sum(left_sum, axis=0, keepdims=True), axis=1, keepdims=True)
    first = lax.broadcasted_iota(jnp.int32, (1, LANES), 1) == 0
    mine = jnp.where(first, load_total, left_total)
    norm_send[...] = mine

    def norm_copy(step):
        return pltpu.make_async_remote_copy(
            src_ref=norm_send,
            dst_ref=norm_recv.at[step - 1],
            send_sem=norm_send_sem.at[step - 1],
            recv_sem=norm_recv_sem.at[step - 1],
            device_id=place(lax.rem(my_id + step, total)),
            device_id_type=MESH,
        )

    def norm_start(step, carry):
        norm_copy(step).start()
        return carry

    def norm_wait(step, carry):
        norm_copy(step).wait()
        return carry

    lax.fori_loop(1, total, norm_start, 0)
    norm_recv[total - 1] = mine
    lax.fori_loop(1, total, norm_wait, 0)

    def add(device, carry):
        slot = lax.rem(my_id - device + total - 1, total)
        return carry + norm_recv[lax.rem(slot + total, total)]

    summed = lax.fori_loop(0, total, add, jnp.zeros((1, LANES), jnp.float32))
    nodes = 3 * ex * ey * ez * total
    norms_ref[...] = jnp.sqrt(summed / nodes)


def on_device(counts, right_side, damage):
    _, ex, ey, ez = right_side.shape
    cz = ez // BLOCK
    wide_x = ex + 2 * HALO
    rows = ey + 16
    flat = wide_x * rows
    wide_y = ey + 2 * HALO
    total = counts[0] * counts[1] * counts[2]
    window = 2 * (-(-COARSE // cz)) + 1
    coarse_rows = -(-(counts[1] + 1) // 8) * 8
    f32 = jnp.float32
    vmem = pltpu.VMEM
    dma = pltpu.SemaphoreType.DMA
    displacement, norms = pl.pallas_call(
        functools.partial(kernel, counts, (ex, ey, ez)),
        out_shape=(
            pltpu.VMEM(right_side.shape, f32),
            pltpu.VMEM((1, LANES), f32),
        ),
        in_specs=[pl.BlockSpec(memory_space=pl.ANY)] * 2,
        out_specs=(
            pl.BlockSpec(memory_space=pltpu.VMEM),
            pl.BlockSpec(memory_space=pltpu.VMEM),
        ),
        scratch_shapes=[
            vmem((2, 4, flat, LANES), f32),
            vmem((2, flat, LANES), f32),
            vmem((2, 3, flat, LANES), f32),
            vmem((2, 3, flat, LANES), f32),
            vmem((ex, ey, LANES), jnp.int32),
            vmem((2, 2, 4, 2, ex, LANES), f32),
            vmem((2, 2, 4, 2, ex, LANES), f32),
            vmem((2, 2, 4, 2, HALO, LANES), f32),
            vmem((2, 2, 4, 2, HALO, LANES), f32),
            vmem((2, 2, 2, 4, 2, 2, LANES), f32),
            vmem((2, 2, 2, 4, 2, 2, LANES), f32),
            vmem((2, 4, HALO, LANES), f32),
            vmem((2, 2, 4, HALO, LANES), f32),
            vmem((2, 2, HALO, LANES), f32),
            vmem((2, 2, 2, HALO, LANES), f32),
            vmem((4, ey, LANES), f32),
            vmem((2, 4, rows, LANES), f32),
            vmem((2, ey, LANES), f32),
            vmem((2, 2, rows, LANES), f32),
            vmem((4, LANES), f32),
            vmem((window, counts[0], counts[1], 4, LANES), f32),
            vmem((counts[0] + 2, 3, 8 + coarse_rows, LANES), f32),
            vmem((2, 3, 9 * rows, LANES), f32),
            vmem((2, 3, 9 * rows, LANES), f32),
            vmem((1, LANES), f32),
            vmem((total, 1, LANES), f32),
            dma((ex + 1,)),
            dma((len(MESSAGES),)),
            dma((len(MESSAGES),)),
            dma((window, counts[0], counts[1])),
            dma((window, counts[0], counts[1])),
            dma((total,)),
            dma((total,)),
            pltpu.SemaphoreType.REGULAR((8, 2)),
        ],
        compiler_params=pltpu.CompilerParams(collective_id=0, has_side_effects=True),
    )(right_side, damage)
    return displacement, norms[0, :2]


def solution(mesh):
    counts = tuple(mesh.shape[axis] for axis in AXES)
    placed = (P(None, "gx", "gy", "gz"), P("gx", "gy", "gz"))
    return jax.shard_map(
        functools.partial(on_device, counts),
        mesh=mesh,
        in_specs=placed,
        out_specs=(P(None, "gx", "gy", "gz"), P()),
        check_vma=False,
    )
```

```python
import functools

import jax
import jax.numpy as jnp
from jax import lax
from jax.experimental import pallas as pl
from jax.experimental.pallas import tpu as pltpu
from jax.sharding import PartitionSpec as P

BLOCK = 16
COARSE = 8
FLOOR_STIFFNESS = 0.05
MASS_TERM = 0.001
COUPLING = 2.5
RELAXATION = 0.6
DIAGONAL = 6.0 + 2.0 * COUPLING
OWN = 1.0 + COUPLING
CROSS = 0.25 * COUPLING
AXES = ("gx", "gy", "gz")
HALO = 4
LANES = 128
MESH = pl.DeviceIdType.MESH
EXACT = lax.Precision.HIGHEST


def messages():
    out = []
    for dx in (-1, 1):
        for part in range(HALO):
            out.append(("x", dx, 0, 0, part))
    for part in range(2):
        for dy in (-1, 1):
            out.append(("y", 0, dy, 0, part))
        for dx in (-1, 1):
            for dy in (-1, 1):
                if part == 1:
                    out.append(("xy", dx, dy, 0, part))
                out.append(("xyn", dx, dy, 0, part))
        if part == 0:
            for dz in (-1, 1):
                for dx in (-1, 0, 1):
                    for dy in (-1, 0, 1):
                        out.append(("z" if dx == 0 else "xz", dx, dy, dz, 0))
    return out


MESSAGES = messages()


def by_two(low, high, body, carry):
    pairs = (high - low) // 2

    def both(trip, carry):
        carry = body(low + 2 * trip, carry)
        return body(low + 2 * trip + 1, carry)

    carry = lax.fori_loop(0, pairs, both, carry)
    return body(high - 1, carry) if (high - low) % 2 else carry


def kernel(
    counts,
    extent,
    load_ref,
    damage_ref,
    out_ref,
    norms_ref,
    base,
    inverse,
    field_a,
    field_b,
    harm,
    y_send,
    y_recv,
    xy_send,
    xy_recv,
    xyn_send,
    xyn_recv,
    yz_send,
    yz_recv,
    xyz_send,
    xyz_recv,
    z_send,
    z_recv,
    xz_send,
    xz_recv,
    coarse_send,
    coarse_recv,
    coarse_w,
    spread_w,
    image_w,
    norm_send,
    norm_recv,
    local_sem,
    send_sem,
    recv_sem,
    coarse_send_sem,
    coarse_recv_sem,
    norm_send_sem,
    norm_recv_sem,
    hello_sem,
):
    count_x, count_y, count_z = counts
    ex, ey, ez = extent
    cz = ez // BLOCK
    total = count_x * count_y * count_z
    wide_x = ex + 2 * HALO
    ypad = 8
    rows = ey + 2 * ypad
    wide_y = ey + 2 * HALO
    first_y = ypad - HALO
    me = tuple(lax.axis_index(axis) for axis in AXES)
    my_id = (me[0] * count_y + me[1]) * count_z + me[2]

    def place(index):
        return (
            index // (count_y * count_z),
            lax.rem(index // count_z, count_y),
            lax.rem(index, count_z),
        )

    load_copies = []
    for x in range(ex):
        target = pl.ds((HALO + x) * rows + ypad, ey)
        load_copies.append(
            pltpu.make_async_copy(load_ref.at[:, x], base.at[0, 0:3, target], local_sem.at[x])
        )
    harm_copy = pltpu.make_async_copy(damage_ref, harm, local_sem.at[ex])
    harm_copy.start()
    for copy in load_copies:
        copy.start()

    barrier = pltpu.get_barrier_semaphore()

    reach = -(-COARSE // cz)
    window = 2 * reach + 1

    def peers(act):
        for dz in range(-reach, reach + 1):
            z = me[2] + dz

            @pl.when((z >= 0) & (z < count_z))
            def _():
                def one(step, carry):
                    if dz == 0:
                        step = step + 1
                    index = lax.rem(me[0] * count_y + me[1] + step, count_x * count_y)
                    act(index // count_y, lax.rem(index, count_y), z, dz)
                    return carry

                lax.fori_loop(0, count_x * count_y - (1 if dz == 0 else 0), one, 0)

    def greet(x, y, z, dz):
        pl.semaphore_signal(barrier, inc=1, device_id=(x, y, z), device_id_type=MESH)

    peers(greet)
    levels = jnp.minimum(me[2] + reach, count_z - 1) - jnp.maximum(me[2] - reach, 0) + 1

    harm_copy.wait()
    for x in range(ex):
        level = 1.0 - harm[x].astype(jnp.float32) / 15.0
        base[0, 3, pl.ds((HALO + x) * rows + ypad, ey)] = (
            level * level * (1.0 - FLOOR_STIFFNESS) + FLOOR_STIFFNESS
        )
    for copy in load_copies:
        copy.wait()

    lane = lax.broadcasted_iota(jnp.int32, (ey, LANES), 1)
    for side in range(2):
        for part in range(2):
            for layer in range(2):
                y = 2 * part + layer if side == 0 else ey - 2 - 2 * part + layer
                for f in range(4):
                    start = HALO * rows + ypad + y
                    for half in range(ex // 8):
                        y_send[side, part, f, layer, pl.ds(8 * half, 8)] = base[
                            0, f, pl.ds(start + 8 * half * rows, 8, stride=rows)
                        ]
                    for xs in range(2):
                        x0 = 0 if xs == 0 else ex - HALO
                        if part == 1:
                            xy_send[xs, side, f, layer] = base[
                                0, f, pl.ds(start + x0 * rows, HALO, stride=rows)
                            ]
                            continue
                        for which in range(2):
                            x0 = 2 * which if xs == 0 else ex - 2 - 2 * which
                            xyn_send[xs, side, which, f, layer] = base[
                                0, f, pl.ds(start + x0 * rows, 2, stride=rows)
                            ]
    for f in range(4):
        packed = None
        for k in range(ex):
            row = base[0, f, pl.ds((HALO + k) * rows + ypad, ey)]
            moved = pltpu.roll(row, (8 * k + HALO) % LANES, 1)
            packed = moved if packed is None else jnp.where(lane // 8 == k, moved, packed)
        z_send[f] = packed
        yz_send[0, f] = packed[:HALO]
        yz_send[1, f] = packed[ey - HALO :]
    for xs in range(2):
        packed = None
        for f in range(4):
            for j in range(HALO):
                x = j if xs == 0 else ex - HALO + j
                k = f * HALO + j
                row = base[0, f, pl.ds((HALO + x) * rows + ypad, ey)]
                moved = pltpu.roll(row, (8 * k + HALO) % LANES, 1)
                packed = moved if packed is None else jnp.where(lane // 8 == k, moved, packed)
        xz_send[xs] = packed
        xyz_send[xs, 0] = packed[:HALO]
        xyz_send[xs, 1] = packed[ey - HALO :]

    pl.semaphore_wait(barrier, levels * count_x * count_y - 1)

    def exists(dx, dy, dz):
        ok = None
        for axis, step in enumerate((dx, dy, dz)):
            if step == 0:
                continue
            here = me[axis] + step
            good = (here >= 0) & (here < counts[axis])
            ok = good if ok is None else ok & good
        return ok

    def describe(number):
        kind, dx, dy, dz, part = MESSAGES[number]
        target = (me[0] + dx, me[1] + dy, me[2] + dz)
        xs, ys, zs = (dx + 1) // 2, (dy + 1) // 2, (dz + 1) // 2
        if kind == "x":
            src_x = HALO + part if dx < 0 else ex + part
            dst_x = HALO + ex + part if dx < 0 else part
            src = base.at[0, :, pl.ds(src_x * rows + ypad, ey)]
            dst = base.at[0, :, pl.ds(dst_x * rows + ypad, ey)]
        elif kind == "y":
            src, dst = y_send.at[ys, part], y_recv.at[1 - ys, part]
        elif kind == "xy":
            src, dst = xy_send.at[xs, ys], xy_recv.at[1 - xs, 1 - ys]
        elif kind == "xyn":
            src, dst = xyn_send.at[xs, ys, part], xyn_recv.at[1 - xs, 1 - ys, part]
        else:
            own = pl.ds(ypad, ey)
            if kind == "z" and dy == 0:
                src, dst = z_send, z_recv.at[1 - zs, :, own]
            elif kind == "z":
                src, dst = yz_send.at[ys], yz_recv.at[1 - zs, 1 - ys]
            elif dy == 0:
                src, dst = xz_send.at[xs], xz_recv.at[1 - xs, 1 - zs, own]
            else:
                src, dst = xyz_send.at[xs, ys], xyz_recv.at[1 - xs, 1 - zs, 1 - ys]
        copy = pltpu.make_async_remote_copy(
            src_ref=src,
            dst_ref=dst,
            send_sem=send_sem.at[number],
            recv_sem=recv_sem.at[number],
            device_id=target,
            device_id_type=MESH,
        )
        return copy, exists(dx, dy, dz), exists(-dx, -dy, -dz)

    for number in range(len(MESSAGES)):
        copy, to_there, _ = describe(number)

        @pl.when(to_there)
        def _():
            copy.start()

    rounds = []
    radius = reach
    while radius < count_z - 1:
        rounds.append(radius)
        radius *= 2

    def hello(number):
        for side, step in enumerate((-rounds[number], rounds[number])):

            @pl.when(exists(0, 0, step))
            def _():
                pl.semaphore_signal(
                    hello_sem.at[number, 1 - side],
                    inc=1,
                    device_id=(me[0], me[1], me[2] + step),
                    device_id_type=MESH,
                )

    def hear(number):
        for side, step in enumerate((-rounds[number], rounds[number])):

            @pl.when(exists(0, 0, step))
            def _():
                pl.semaphore_wait(hello_sem.at[number, side], 1)

    if rounds:
        hello(0)

    def wait_for(part, send):
        for number, message in enumerate(MESSAGES):
            far = message[0] in ("y", "xy", "xyn") and message[4] == 1
            if send and (message[0] == "x") != (part == 0):
                continue
            if not send and far != (part == 1):
                continue
            copy, to_there, from_there = describe(number)

            @pl.when(to_there if send else from_there)
            def _():
                if send:
                    copy.wait_send()
                else:
                    copy.wait_recv()

    def unpack_y(part):
        for side in range(2):
            for layer in range(2):
                y = (
                    ypad - 2 - 2 * part + layer
                    if side == 0
                    else ypad + ey + 2 * part + layer
                )
                for f in range(4):
                    for half in range(ex // 8):
                        base[
                            0, f, pl.ds((HALO + 8 * half) * rows + y, 8, stride=rows)
                        ] = y_recv[side, part, f, layer, pl.ds(8 * half, 8)]
                    near_y = ypad - 2 + layer if side == 0 else ypad + ey + layer
                    for xs in range(2):
                        x0 = 0 if xs == 0 else HALO + ex
                        if part == 1:
                            base[0, f, pl.ds(x0 * rows + y, HALO, stride=rows)] = xy_recv[
                                xs, side, f, layer
                            ]
                        x0 = 2 - 2 * part if xs == 0 else HALO + ex + 2 * part
                        base[0, f, pl.ds(x0 * rows + near_y, 2, stride=rows)] = xyn_recv[
                            xs, side, part, f, layer
                        ]

    def unpack_z():
        lane_rows = lax.broadcasted_iota(jnp.int32, (rows, LANES), 1)
        lower = lax.rem(lane_rows, 8) < HALO
        for zs in range(2):
            for ys in range(2):
                edge = pl.ds(first_y if ys == 0 else ypad + ey, HALO)
                for f in range(4):
                    z_recv[zs, f, edge] = yz_recv[zs, ys, f]
                for xs in range(2):
                    xz_recv[xs, zs, edge] = xyz_recv[xs, zs, ys]
        for f in range(4):
            merged = jnp.where(lower, z_recv[0, f], z_recv[1, f])
            for k in range(ex):
                base[1, f, pl.ds((HALO + k) * rows, rows)] = pltpu.roll(
                    merged, (2 * LANES - 8 * k - HALO) % LANES, 1
                )
        for xs in range(2):
            merged = jnp.where(lower, xz_recv[xs, 0], xz_recv[xs, 1])
            for f in range(4):
                for j in range(HALO):
                    k = f * HALO + j
                    x = j if xs == 0 else HALO + ex + j
                    base[1, f, pl.ds(x * rows, rows)] = pltpu.roll(
                        merged, (2 * LANES - 8 * k - HALO) % LANES, 1
                    )

    lane = lax.broadcasted_iota(jnp.int32, (wide_y, LANES), 1)
    row_y = lax.broadcasted_iota(jnp.int32, (wide_y, LANES), 0)
    at_y = me[1] * ey + row_y - HALO
    good_y = (at_y >= 0) & (at_y < ey * count_y)
    good_halo = (
        good_y
        & ((me[2] > 0) | (lane < LANES // 2))
        & ((me[2] < count_z - 1) | (lane >= LANES // 2))
    )
    goods = (good_y, good_halo)

    def at(x, dy=0, own=False):
        if own:
            return pl.ds(x * rows + ypad + dy, ey)
        return pl.ds(x * rows + first_y + dy, wide_y)

    def prepare(x, carry):
        at_x = me[0] * ex + x - HALO
        good_x = (at_x >= 0) & (at_x < ex * count_x)
        for t in range(2):
            good = goods[t] & good_x
            g = jnp.where(good, base[t, 3, at(x)], 1.0)
            base[t, 3, at(x)] = g
            inv = jnp.where(good, RELAXATION / (g * DIAGONAL + MASS_TERM), 0.0)
            inverse[t, at(x)] = inv
            for c in range(3):
                load = jnp.where(good, base[t, c, at(x)], 0.0)
                base[t, c, at(x)] = load
                field_a[t, c, at(x)] = load * inv
        return carry

    def image(field, x, own=False):
        parts = [[None] * 3, [None] * 3]
        ups = [[None] * 3, [None] * 3]
        downs = [[None] * 3, [None] * 3]
        for t in range(2):

            def load(c, ox, oy):
                return field[t, c, at(x + ox, oy, own)]

            centre = [load(c, 0, 0) for c in range(3)]
            x_up = [load(c, 1, 0) for c in range(3)]
            x_down = [load(c, -1, 0) for c in range(3)]
            y_up = [load(c, 0, 1) for c in range(3)]
            y_down = [load(c, 0, -1) for c in range(3)]

            def corners(c):
                return (load(c, 1, 1) - load(c, 1, -1)) - (load(c, -1, 1) - load(c, -1, -1))

            sum_x = [x_up[c] + x_down[c] for c in range(3)]
            sum_y = [y_up[c] + y_down[c] for c in range(3)]
            parts[t][0] = DIAGONAL * centre[0] - OWN * sum_x[0] - sum_y[0] - CROSS * corners(1)
            parts[t][1] = DIAGONAL * centre[1] - sum_x[1] - OWN * sum_y[1] - CROSS * corners(0)
            parts[t][2] = DIAGONAL * centre[2] - sum_x[2] - sum_y[2]
            tilt_x = CROSS * (x_up[2] - x_down[2])
            tilt_y = CROSS * (y_up[2] - y_down[2])
            tilt_z = CROSS * ((x_up[0] - x_down[0]) + (y_up[1] - y_down[1]))
            own_z = OWN * centre[2]
            ups[t] = [centre[0] + tilt_x, centre[1] + tilt_y, own_z + tilt_z]
            downs[t] = [centre[0] - tilt_x, centre[1] - tilt_y, own_z - tilt_z]
        out = [[None] * 3, [None] * 3]
        lanes = lax.broadcasted_iota(jnp.int32, parts[0][0].shape, 1)
        first_lane = lanes == 0
        last_lane = lanes == LANES - 1
        for c in range(3):
            up = [pltpu.roll(ups[t][c], LANES - 1, 1) for t in range(2)]
            down = [pltpu.roll(downs[t][c], 1, 1) for t in range(2)]
            for t in range(2):
                beside = jnp.where(last_lane, up[1 - t], up[t]) + jnp.where(
                    first_lane, down[1 - t], down[t]
                )
                out[t][c] = parts[t][c] - beside
        return out

    def residual(field, x, tiles, own=False):
        images = image(field, x, own)
        out = []
        here = at(x, 0, own)
        for t in tiles:
            g = base[t, 3, here]
            out.append(
                [
                    base[t, c, here] - (g * images[t][c] + MASS_TERM * field[t, c, here])
                    for c in range(3)
                ]
            )
        return out

    def sweep(source, target, low, high):
        def one(x, carry):
            left = residual(source, x, (0, 1))
            for t in range(2):
                inv = inverse[t, at(x)]
                for c in range(3):
                    target[t, c, at(x)] = source[t, c, at(x)] + inv * left[t][c]
            return carry

        by_two(low, high, one, 0)

    def fold(value):
        return jnp.sum(value.reshape(ey // 8, 8, LANES), axis=0)

    zero = jnp.zeros((8, LANES), jnp.float32)

    wait_for(0, False)
    wait_for(0, True)
    unpack_y(0)
    unpack_z()
    by_two(2, wide_x - 2, prepare, 0)
    sweep(field_a, field_b, 3, wide_x - 3)

    def restrict(x, carry):
        left = residual(field_b, x, (0,), True)[0]
        sums = [carry[c] + fold(left[c]) for c in range(3)]
        sums.append(carry[3] + fold(base[0, 3, at(x, 0, True)]))
        return tuple(sums)

    sums = by_two(HALO, HALO + ex, restrict, (zero,) * 4)
    stacked = jnp.concatenate([jnp.sum(s, axis=0, keepdims=True) for s in sums] + [zero[:4]], axis=0)
    source_lane = lax.broadcasted_iota(jnp.int32, (LANES, LANES), 0)
    target_lane = lax.broadcasted_iota(jnp.int32, (LANES, LANES), 1)
    gather = (source_lane // BLOCK == lax.rem(target_lane, cz)).astype(jnp.float32)
    grouped = jnp.dot(stacked, gather, precision=EXACT, preferred_element_type=jnp.float32)
    coarse_send[...] = grouped[:4]

    def coarse_copy(x, y, z, dz):
        return pltpu.make_async_remote_copy(
            src_ref=coarse_send,
            dst_ref=coarse_recv.at[reach - dz, me[0], me[1]],
            send_sem=coarse_send_sem.at[reach + dz, x, y],
            recv_sem=coarse_recv_sem.at[reach - dz, me[0], me[1]],
            device_id=(x, y, z),
            device_id_type=MESH,
        )

    def coarse_wait(x, y, z, dz):
        pltpu.make_async_remote_copy(
            src_ref=coarse_send,
            dst_ref=coarse_recv.at[reach + dz, x, y],
            send_sem=coarse_send_sem.at[reach + dz, x, y],
            recv_sem=coarse_recv_sem.at[reach + dz, x, y],
            device_id=(x, y, z),
            device_id_type=MESH,
        ).wait()

    peers(lambda x, y, z, dz: coarse_copy(x, y, z, dz).start())
    coarse_recv[reach, me[0], me[1]] = grouped[:4]

    wait_for(1, False)
    unpack_y(1)
    by_two(0, wide_x, prepare, 0)
    sweep(field_a, field_b, 1, wide_x - 1)
    sweep(field_b, field_a, 2, wide_x - 2)

    def load_squares(x, carry):
        loads = [base[0, c, at(x, 0, True)] for c in range(3)]
        return carry + fold(sum(value * value for value in loads))

    load_sum = by_two(HALO, HALO + ex, load_squares, zero)
    wait_for(1, True)
    for number in range(len(rounds)):
        if number > 0:
            hello(number)
        hear(number)
    peers(coarse_wait)

    coarse_rows = -(-(count_y + 1) // 8) * 8
    lane_c = lax.broadcasted_iota(jnp.int32, (coarse_rows, LANES), 1)
    row_c = lax.broadcasted_iota(jnp.int32, (coarse_rows, LANES), 0)
    at_z = me[2] * cz - reach * cz + lane_c
    valid = (
        (row_c < count_y) & (at_z >= 0) & (at_z < cz * count_z) & (lane_c < window * cz)
    )
    slab = [[None] * 4 for _ in range(count_x)]
    for x in range(count_x):
        for c in range(4):
            value = None
            for w in range(window):
                column = jnp.concatenate(
                    [coarse_recv[w, x, y, c : c + 1] for y in range(count_y)]
                    + [jnp.zeros((coarse_rows - count_y, LANES), jnp.float32)],
                    axis=0,
                )
                value = column if value is None else jnp.where(lane_c // cz == w, column, value)
            slab[x][c] = jnp.where(valid, value, 0.0)
    mass = BLOCK**3 * MASS_TERM
    factor = [slab[x][3] * (BLOCK**2 / BLOCK**3) for x in range(count_x)]
    relax = [
        jnp.where(valid, RELAXATION / (factor[x] * DIAGONAL + mass), 0.0) for x in range(count_x)
    ]
    nothing = jnp.zeros((coarse_rows, LANES), jnp.float32)
    w = [[slab[x][c] * relax[x] for c in range(3)] for x in range(count_x)]

    def y_shift(value, step):
        return pltpu.roll(value, step % coarse_rows, 0)

    def z_shift(value, step):
        return pltpu.roll(value, step % LANES, 1)

    for repeat in range(COARSE - 1):
        fresh = []
        for x in range(count_x):
            here = w[x]
            above = w[x + 1] if x + 1 < count_x else [nothing] * 3
            below = w[x - 1] if x > 0 else [nothing] * 3
            sum_x = [above[c] + below[c] for c in range(3)]
            diff_x = [above[c] - below[c] for c in range(3)]
            y_up = [y_shift(here[c], -1) for c in range(3)]
            y_down = [y_shift(here[c], 1) for c in range(3)]
            sum_y = [y_up[c] + y_down[c] for c in range(3)]
            diff_y = [y_up[c] - y_down[c] for c in range(3)]
            corner_x = y_shift(diff_x[1], -1) - y_shift(diff_x[1], 1)
            corner_y = y_shift(diff_x[0], -1) - y_shift(diff_x[0], 1)
            tilt = [CROSS * diff_x[2], CROSS * diff_y[2], CROSS * (diff_x[0] + diff_y[1])]
            own = [here[0], here[1], OWN * here[2]]
            beside = [z_shift(own[c] + tilt[c], -1) + z_shift(own[c] - tilt[c], 1) for c in range(3)]
            flat = [
                DIAGONAL * here[0] - OWN * sum_x[0] - sum_y[0] - CROSS * corner_x - beside[0],
                DIAGONAL * here[1] - sum_x[1] - OWN * sum_y[1] - CROSS * corner_y - beside[1],
                DIAGONAL * here[2] - sum_x[2] - sum_y[2] - beside[2],
            ]
            fresh.append(
                [
                    here[c] + relax[x] * (slab[x][c] - (factor[x] * flat[c] + mass * here[c]))
                    for c in range(3)
                ]
            )
        w = fresh

    for x in range(count_x + 2):
        for c in range(3):
            inside = 1 <= x <= count_x
            coarse_w[x, c, pl.ds(0, 8)] = jnp.zeros((8, LANES), jnp.float32)
            coarse_w[x, c, pl.ds(8, coarse_rows)] = w[x - 1][c] if inside else nothing
    widen_core = (source_lane == reach * cz + target_lane // BLOCK).astype(jnp.float32)
    widen_halo = (
        source_lane == jnp.where(target_lane < LANES // 2, (reach + 1) * cz, reach * cz - 1)
    ).astype(jnp.float32)
    for xc in range(3):
        for c in range(3):
            cells = [coarse_w[me[0] + xc, c, pl.ds(7 + me[1] + k, 1)] for k in range(3)]
            stacked = jnp.concatenate(cells + [zero[:5]], axis=0)
            for t, matrix in enumerate((widen_core, widen_halo)):
                wide = jnp.dot(stacked, matrix, precision=EXACT, preferred_element_type=jnp.float32)
                low = jnp.broadcast_to(wide[0:1], (wide_y, LANES))
                mid = jnp.broadcast_to(wide[1:2], (wide_y, LANES))
                top = jnp.broadcast_to(wide[2:3], (wide_y, LANES))
                wide = jnp.where(row_y < HALO, low, jnp.where(row_y < HALO + ey, mid, top))
                for plane in range(3):
                    spread_w[t, c, pl.ds((3 * xc + plane) * rows + first_y, wide_y)] = wide
    for plane in range(1, 8):
        images = image(spread_w, plane)
        for t in range(2):
            for c in range(3):
                image_w[t, c, at(plane)] = images[t][c]

    def correct(x, carry):
        kind = (
            1
            + (x >= HALO - 1).astype(jnp.int32)
            + (x >= HALO).astype(jnp.int32)
            + (x >= HALO + 1).astype(jnp.int32)
            + (x >= HALO + ex - 1).astype(jnp.int32)
            + (x >= HALO + ex).astype(jnp.int32)
            + (x >= HALO + ex + 1).astype(jnp.int32)
        )
        for t in range(2):
            inv = inverse[t, at(x)]
            g = base[t, 3, at(x)]
            for c in range(3):
                added = spread_w[t, c, at(kind)]
                field_a[t, c, at(x)] = (
                    field_a[t, c, at(x)]
                    + added
                    - inv * (g * image_w[t, c, at(kind)] + MASS_TERM * added)
                )
        return carry

    by_two(2, wide_x - 2, correct, 0)
    sweep(field_a, field_b, 3, wide_x - 3)

    def squares(x, carry):
        left = residual(field_b, x, (0,), True)[0]
        for c in range(3):
            out_ref[c, x - HALO] = field_b[0, c, at(x, 0, True)]
        return carry + fold(sum(value * value for value in left))

    left_sum = by_two(HALO, HALO + ex, squares, zero)
    load_total = jnp.sum(jnp.sum(load_sum, axis=0, keepdims=True), axis=1, keepdims=True)
    left_total = jnp.sum(jnp.sum(left_sum, axis=0, keepdims=True), axis=1, keepdims=True)
    first = lax.broadcasted_iota(jnp.int32, (1, LANES), 1) == 0
    mine = jnp.where(first, load_total, left_total)
    norm_send[...] = mine

    def norm_copy(step):
        return pltpu.make_async_remote_copy(
            src_ref=norm_send,
            dst_ref=norm_recv.at[step - 1],
            send_sem=norm_send_sem.at[step - 1],
            recv_sem=norm_recv_sem.at[step - 1],
            device_id=place(lax.rem(my_id + step, total)),
            device_id_type=MESH,
        )

    def norm_start(step, carry):
        norm_copy(step).start()
        return carry

    def norm_wait(step, carry):
        norm_copy(step).wait()
        return carry

    lax.fori_loop(1, total, norm_start, 0)
    norm_recv[total - 1] = mine
    lax.fori_loop(1, total, norm_wait, 0)

    def add(device, carry):
        slot = lax.rem(my_id - device + total - 1, total)
        return carry + norm_recv[lax.rem(slot + total, total)]

    summed = lax.fori_loop(0, total, add, jnp.zeros((1, LANES), jnp.float32))
    nodes = 3 * ex * ey * ez * total
    norms_ref[...] = jnp.sqrt(summed / nodes)


def on_device(counts, right_side, damage):
    _, ex, ey, ez = right_side.shape
    cz = ez // BLOCK
    wide_x = ex + 2 * HALO
    rows = ey + 16
    flat = wide_x * rows
    wide_y = ey + 2 * HALO
    total = counts[0] * counts[1] * counts[2]
    window = 2 * (-(-COARSE // cz)) + 1
    coarse_rows = -(-(counts[1] + 1) // 8) * 8
    f32 = jnp.float32
    vmem = pltpu.VMEM
    dma = pltpu.SemaphoreType.DMA
    displacement, norms = pl.pallas_call(
        functools.partial(kernel, counts, (ex, ey, ez)),
        out_shape=(
            pltpu.VMEM(right_side.shape, f32),
            pltpu.VMEM((1, LANES), f32),
        ),
        in_specs=[pl.BlockSpec(memory_space=pl.ANY)] * 2,
        out_specs=(
            pl.BlockSpec(memory_space=pltpu.VMEM),
            pl.BlockSpec(memory_space=pltpu.VMEM),
        ),
        scratch_shapes=[
            vmem((2, 4, flat, LANES), f32),
            vmem((2, flat, LANES), f32),
            vmem((2, 3, flat, LANES), f32),
            vmem((2, 3, flat, LANES), f32),
            vmem((ex, ey, LANES), jnp.int32),
            vmem((2, 2, 4, 2, ex, LANES), f32),
            vmem((2, 2, 4, 2, ex, LANES), f32),
            vmem((2, 2, 4, 2, HALO, LANES), f32),
            vmem((2, 2, 4, 2, HALO, LANES), f32),
            vmem((2, 2, 2, 4, 2, 2, LANES), f32),
            vmem((2, 2, 2, 4, 2, 2, LANES), f32),
            vmem((2, 4, HALO, LANES), f32),
            vmem((2, 2, 4, HALO, LANES), f32),
            vmem((2, 2, HALO, LANES), f32),
            vmem((2, 2, 2, HALO, LANES), f32),
            vmem((4, ey, LANES), f32),
            vmem((2, 4, rows, LANES), f32),
            vmem((2, ey, LANES), f32),
            vmem((2, 2, rows, LANES), f32),
            vmem((4, LANES), f32),
            vmem((window, counts[0], counts[1], 4, LANES), f32),
            vmem((counts[0] + 2, 3, 8 + coarse_rows, LANES), f32),
            vmem((2, 3, 9 * rows, LANES), f32),
            vmem((2, 3, 9 * rows, LANES), f32),
            vmem((1, LANES), f32),
            vmem((total, 1, LANES), f32),
            dma((ex + 1,)),
            dma((len(MESSAGES),)),
            dma((len(MESSAGES),)),
            dma((window, counts[0], counts[1])),
            dma((window, counts[0], counts[1])),
            dma((total,)),
            dma((total,)),
            pltpu.SemaphoreType.REGULAR((8, 2)),
        ],
        compiler_params=pltpu.CompilerParams(collective_id=0, has_side_effects=True),
    )(right_side, damage)
    return displacement, norms[0, :2]


def solution(mesh):
    counts = tuple(mesh.shape[axis] for axis in AXES)
    placed = (P(None, "gx", "gy", "gz"), P("gx", "gy", "gz"))
    return jax.shard_map(
        functools.partial(on_device, counts),
        mesh=mesh,
        in_specs=placed,
        out_specs=(P(None, "gx", "gy", "gz"), P()),
        check_vma=False,
    )
```
